256 devices in a mesh: row: 4 (over x_hi, core), col: 4 (over y), depth: 16 (over z, x_lo).
Axes of the slice: x: 4 (x_hi: 2, x_lo: 2; x = x_hi * 2 + x_lo), y: 4, z: 8, core: 2. Of those that a mesh axis runs over, the one named last changes fastest.
Arguments:
- acts: bfloat16 [2048, 32768], P('depth', 'row'), may hold values from -6 to 6
- act_mask: int32 [2048, 256], P('depth', 'row'), may hold values 0 or 1
- w1: bfloat16 [256, 32, 128, 128], P(('row', 'depth'), 'col'), may hold values from -0.09375 to 0.09375
- cols1: int32 [256, 32], P('row', 'col'), may hold values from 0 to 255, as said below
- bias1: float32 [32768], P('col'), may hold values from -3 to 3
- mask2: int32 [2048, 256], P('depth', 'col'), may hold values 0 or 1
- w2: bfloat16 [256, 32, 128, 128], P(('col', 'depth'), 'row'), may hold values from -0.1875 to 0.1875
- cols2: int32 [256, 32], P('col', 'row'), may hold values from 0 to 255, as said below
- bias2: float32 [32768], P(('row', 'col')), may hold values from -3 to 3
Outputs:
- result: bfloat16 [2048, 32768], P('depth', ('row', 'col'))
The draws below stay inside these ranges and needn't reach their ends.
Inputs may be any that keep to these rules, and one draw needn't show every extreme that they name: `cols1`: in each of the 256 block rows the 32 entries name different block columns, and for every g the entries g * 8 to g * 8 + 7 lie among block columns g * 64 to g * 64 + 63. `cols2`: in each of the 256 block rows the 32 entries name different block columns, and for every g the entries g * 8 to g * 8 + 7 lie among block columns g * 64 to g * 64 + 63.
All inputs are finite; a program needn't handle non-finite values. No bound on the sum of `act_mask` or of `mask2` on one device may be relied on, other than what follows from the above.
Results may differ from the reference program's by a relative error of at most 0.0047.
Values may be sent and summed in bfloat16 or wider, within the bound.
A program may use at most 128 MiB of HBM per device.

```python
import jax
import jax.numpy as jnp
from jax import lax

N = 32768
BS = 128
K = 32
NB = 256
NB_COL = 64
NB_ROW = 64
KC = 8
KR = 8
M = 2048


def pattern(key, extent, per_group):
    groups = NB // extent
    score_values = jax.random.randint(key, (NB, groups, extent), 0, 1 << 20, dtype=jnp.int32)
    score_values = score_values * extent + jnp.arange(extent, dtype=jnp.int32)
    ranked = jnp.argsort(score_values, axis=-1)[:, :, :per_group].astype(jnp.int32)
    placed = ranked + (jnp.arange(groups, dtype=jnp.int32) * extent)[None, :, None]
    return placed.reshape(NB, groups * per_group).astype(jnp.int32)


def draw_cols1(key, part):
    return pattern(jax.random.fold_in(key, 1), NB_COL, KC)


def draw_cols2(key, part):
    return pattern(jax.random.fold_in(key, 2), NB_ROW, KR)


def with_ends(entries, own_key, smallest, high):
    index_at = [jax.random.randint(jax.random.fold_in(own_key, axis), (), 0, length) for axis, length in enumerate(entries.shape)]
    longest = entries.shape.index(max(entries.shape))
    neighbour = index_at[:longest] + [(index_at[longest] + 1) % entries.shape[longest]] + index_at[longest + 1:]
    return entries.at[tuple(index_at)].set(smallest).at[tuple(neighbour)].set(high)


def level_of(stream_key, shape, cuts, low, high):
    level = 1.0
    for position, blocks in cuts:
        draws = jax.random.uniform(jax.random.fold_in(jax.random.fold_in(stream_key, 6), position), (blocks,), jnp.float32, low / len(cuts), high / len(cuts))
        level = level * jnp.repeat(jnp.exp(draws), shape[position] // blocks).reshape((-1,) + (1,) * (len(shape) - 1 - position))
    return level


def normal_values(rng, shape, scale, most, pieces=(), kind=jnp.bfloat16):
    drawn = jax.random.normal(rng, shape, jnp.float32) * scale
    if len(pieces) > 0:
        drawn = level_of(rng, shape, pieces, -0.22, 0.18) * drawn
    return jnp.clip(drawn, min=-most, max=most).astype(kind)


def setup_inputs(seed: int = 0) -> dict:
    arg_keys = jax.random.split(jax.random.key(seed), 10)
    return {
        "acts": normal_values(arg_keys[0], (M, N), 1.0, 6.0, ((0, 16), (1, 4))),
        "act_mask": with_ends((jax.random.randint(arg_keys[1], (M, NB), 0, 4) < 3).astype(jnp.int32), jax.random.fold_in(arg_keys[1], 1), 0, 1),
        "w1": normal_values(arg_keys[2], (NB, K, BS, BS), (K * BS) ** -0.5, 0.09375, ((0, 64), (1, 4))),
        "cols1": draw_cols1(jax.random.fold_in(arg_keys[9], 71), 0),
        "bias1": normal_values(arg_keys[4], (N,), 0.5, 3.0, ((0, 4),), jnp.float32),
        "mask2": with_ends((jax.random.randint(arg_keys[5], (M, NB), 0, 4) < 3).astype(jnp.int32), jax.random.fold_in(arg_keys[5], 1), 0, 1),
        "w2": normal_values(arg_keys[6], (NB, K, BS, BS), (K * BS // 4) ** -0.5, 0.1875, ((0, 64), (1, 4))),
        "cols2": draw_cols2(jax.random.fold_in(arg_keys[9], 71), 0),
        "bias2": normal_values(arg_keys[8], (N,), 0.5, 3.0, ((0, 16),), jnp.float32),
    }


def dense_layer(inputs, weights, targets, bias):
    blocks_in = inputs.reshape(M, NB, BS).astype(jnp.float32)

    def advance(running_total, block_row):
        incoming_rows = blocks_in[:, block_row]
        tiles = weights[block_row].astype(jnp.float32)
        product = jnp.einsum("mb,kbc->mkc", incoming_rows, tiles)
        return running_total.at[:, targets[block_row]].add(product), None

    start_value = jnp.zeros((M, NB, BS), jnp.float32)
    summed, unused = lax.scan(advance, start_value, jnp.arange(NB, dtype=jnp.int32))
    return jnp.maximum(summed + bias.reshape(NB, BS), 0.0)


def reference(acts, act_mask, w1, cols1, bias1, mask2, w2, cols2, bias2):
    masked = acts.reshape(M, NB, BS) * act_mask[:, :, None].astype(jnp.bfloat16)
    masked = masked.reshape(M, N)
    first = dense_layer(masked, w1, cols1, bias1)
    hidden = (first * mask2[:, :, None].astype(jnp.float32)).astype(jnp.bfloat16)
    second = dense_layer(hidden.reshape(M, N), w2, cols2, bias2)
    return second.astype(jnp.bfloat16).reshape(M, N)
```

```python
import functools

import jax
import jax.numpy as jnp
from jax import lax
from jax.experimental import pallas as pl
from jax.experimental.pallas import tpu as pltpu
from jax.sharding import Mesh
from jax.sharding import PartitionSpec as P

AXES = ("xh", "core", "y", "z", "xl")
DEPTH = ("z", "xl")
ROW = ("xh", "core")
SWAP = ((0, 0), (1, 2), (2, 1), (3, 3))
BF16, F32 = jnp.bfloat16, jnp.float32


def flip(i):
    return i + 1 - 2 * lax.rem(i, 2)


def xor4(i, j):
    low = lax.rem(i + j, 2)
    high = lax.rem(i // 2 + j // 2, 2)
    return high * 2 + low


def product_kernel(load, store, rows_in_step, pos_ref, core_ref, x_ref, w_ref, keep_ref, send_ref, acc_ref):
    step = pl.program_id(0)
    columns, entries = acc_ref.shape[0], w_ref.shape[1]

    @pl.when(step == 0)
    def _():
        @pl.loop(0, columns)
        def _(c):
            acc_ref[c] = jnp.zeros(acc_ref.shape[1:], F32)

    for b in range(rows_in_step):
        i = step * rows_in_step + b
        lhs = load(x_ref, i)
        for k in range(0, entries, 2):
            rhs = jnp.concatenate([w_ref[b, k], w_ref[b, k + 1]], axis=1)
            out = jnp.dot(lhs, rhs, preferred_element_type=F32)
            width = out.shape[1] // 2
            acc_ref[pos_ref[i, k]] += out[:, :width]
            acc_ref[pos_ref[i, k + 1]] += out[:, width:]

    @pl.when(step == pl.num_programs(0) - 1)
    def _():
        store(core_ref[0], acc_ref, keep_ref, send_ref)


def store_columns(core, acc_ref, keep_ref, send_ref):
    half = keep_ref.shape[0]

    @pl.loop(0, half)
    def _(c):
        keep_ref[c] = acc_ref[c]
        send_ref[c] = acc_ref[c + half].astype(BF16)


def store_rows(core, acc_ref, keep_ref, send_ref):
    rows = keep_ref.shape[1]
    mine = pl.multiple_of(core * rows, rows)
    theirs = pl.multiple_of((1 - core) * rows, rows)

    @pl.loop(0, keep_ref.shape[0])
    def _(c):
        keep_ref[c] = acc_ref[c, pl.ds(mine, rows), :]
        send_ref[c] = acc_ref[c, pl.ds(theirs, rows), :].astype(BF16)


def load_columns(x_ref, i):
    return x_ref[:, pl.ds(pl.multiple_of(i * 128, 128), 128)]


def load_blocks(x_ref, i):
    return x_ref[i]


def products(x, w, pos, core, load, store, out_shape, rows, columns, name):
    block_rows, entries, bs, _ = w.shape
    rows_in_step = 4
    whole = lambda shape: pl.BlockSpec(shape, lambda s, *_: (0,) * len(shape))
    return pl.pallas_call(
        functools.partial(product_kernel, load, store, rows_in_step),
        out_shape=(jax.ShapeDtypeStruct(out_shape, F32), jax.ShapeDtypeStruct(out_shape, BF16)),
        grid_spec=pltpu.PrefetchScalarGridSpec(
            num_scalar_prefetch=2,
            grid=(block_rows // rows_in_step,),
            in_specs=[
                whole(x.shape),
                pl.BlockSpec((rows_in_step, entries, bs, bs), lambda s, *_: (s, 0, 0, 0)),
            ],
            out_specs=[whole(out_shape), whole(out_shape)],
            scratch_shapes=[pltpu.VMEM((columns, rows, bs), F32)],
        ),
        compiler_params=pltpu.CompilerParams(vmem_limit_bytes=48 << 20),
        cost_estimate=pl.CostEstimate(
            flops=2 * rows * block_rows * entries * bs * bs,
            bytes_accessed=w.size * 2 + x.size * 2 + 6 * out_shape[0] * out_shape[1] * bs,
            transcendentals=0,
        ),
        name=name,
    )(pos, core, x, w)


def remote(src, dst, sems, n, device):
    return pltpu.make_async_remote_copy(
        src_ref=src,
        dst_ref=dst,
        send_sem=sems.at[0, n],
        recv_sem=sems.at[1, n],
        device_id=device,
        device_id_type=pl.DeviceIdType.MESH,
    )


def greet(devices):
    barrier = pltpu.get_barrier_semaphore()
    for device in devices:
        pl.semaphore_signal(barrier, inc=1, device_id=device, device_id_type=pl.DeviceIdType.MESH)
    pl.semaphore_wait(barrier, len(devices))


FIRST = ((2, 1), (2, 3))
LANDS = ((3, 0), (1, 0))


def reduce_scatter(other, near, keep, send, got, out1, in1, out2, in2, sems, finish):
    half = keep.shape[1] // 2

    def part(ref, g, h):
        return ref.at[g, pl.ds(h * half, half)]

    exchanged = {}
    order = [(2, 0), (2, 1), (1, 0), (3, 1), (3, 0), (1, 1), (0, 0), (0, 1)]
    for n, (g, h) in enumerate(order):
        exchanged[g, h] = remote(part(send, g, h), part(got, g, h), sems, n, other)
        exchanged[g, h].start()

    def both(g, h, c):
        return keep[g, h * half + c] + got[g, h * half + c].astype(F32)

    firsts = {}
    for s in range(2):
        for h in range(2):
            g = FIRST[h][s]
            exchanged[g, h].wait_recv()

            @pl.loop(0, half)
            def _(c):
                out1[h, s, c] = both(g, h, c).astype(BF16)

            firsts[h, s] = remote(out1.at[h, s], in1.at[h, s], sems, 8 + 2 * h + s, near[h])
            firsts[h, s].start()
    seconds = {}
    for h in range(2):
        g = LANDS[h][0]
        exchanged[g, h].wait_recv()
        firsts[h, 0].wait_recv()

        @pl.loop(0, half)
        def _(c):
            out2[h, c] = (both(g, h, c) + in1[h, 0, c].astype(F32)).astype(BF16)

        seconds[h] = remote(out2.at[h], in2.at[h], sems, 12 + h, near[1 - h])
        seconds[h].start()
    for h in range(2):
        exchanged[0, h].wait_recv()
        firsts[h, 1].wait_recv()
        seconds[h].wait_recv()
        finish(h, lambda c: both(0, h, c) + in1[h, 1, c].astype(F32) + in2[h, c].astype(F32))
    for copy in [*exchanged.values(), *firsts.values(), *seconds.values()]:
        copy.wait_send()


def hidden_kernel(keep, send, bias, mask, hid, got, out1, in1, out2, in2, sems):
    xh, core, xl = lax.axis_index("xh"), lax.axis_index("core"), lax.axis_index("xl")
    x = xh * 2 + xl
    other = {"core": 1 - core}
    near = ({"xl": 1 - xl}, {"xh": 1 - xh, "xl": 1 - xl})
    index = (flip(x), 3 - x)
    greet((other, *near))
    half = keep.shape[1] // 2

    def piece(chip, h):
        return hid.at[chip, pl.ds(h * half, half)]

    copies = []

    def spread(chip, h, to, n):
        copy = remote(piece(chip, h), piece(chip, h), sems, n, near[to])
        copy.start()
        copies.append(copy)
        return copy

    given = {}

    def finish(h, total):
        for c in range(half):
            n = h * half + c
            value = jnp.maximum(total(c) + bias[pl.ds(n, 1), :], 0.0) * mask[n].astype(F32)
            hid[x, n] = value.astype(BF16)
        for to in (1 - h, h):
            given[h, to] = spread(x, h, to, 14 + 2 * h + to)

    reduce_scatter(other, near, keep, send, got, out1, in1, out2, in2, sems, finish)
    for h in range(2):
        given[h, 1 - h].wait_recv()
        spread(index[1 - h], h, h, 18 + h)
    for h in range(2):
        given[h, h].wait_recv()
    for copy in copies[4:]:
        copy.wait_recv()
    for copy in copies:
        copy.wait_send()


def result_kernel(keep, send, bias, out, got, out1, in1, out2, in2, fin, sems):
    core, y, xl = lax.axis_index("core"), lax.axis_index("y"), lax.axis_index("xl")
    other = {"core": 1 - core}
    near = ({"y": flip(y)}, {"y": 3 - y})
    home = {"core": 1 - core, "xl": 1 - xl}
    away = xl != core
    greet((other, *near, home))
    half = keep.shape[1] // 2
    bs = keep.shape[-1]

    def back(h):
        piece = pl.ds(h * half * bs, half * bs)
        return remote(fin.at[:, piece], out.at[:, piece], sems, 14 + h, home)

    def finish(h, total):
        for c in range(half):
            n = h * half + c
            value = jnp.maximum(total(c) + bias[pl.ds(n, 1), :], 0.0)
            fin[:, n * bs : (n + 1) * bs] = value.astype(BF16)

        @pl.when(away)
        def _():
            back(h).start()

    reduce_scatter(other, near, keep, send, got, out1, in1, out2, in2, sems, finish)

    @pl.when(away)
    def _():
        for h in range(2):
            back(h).wait()

    @pl.when(jnp.logical_not(away))
    def _():
        out[...] = fin[...]


def summed(kernel, keep, send, operands, out_shape, extra, n_sems, collective_id, name):
    chips, blocks, rows, bs = keep.shape
    half = (blocks // 2, rows, bs)
    vmem = pl.BlockSpec(memory_space=pltpu.VMEM)
    return pl.pallas_call(
        kernel,
        out_shape=jax.ShapeDtypeStruct(out_shape, BF16),
        in_specs=[vmem] * (2 + len(operands)),
        out_specs=vmem,
        scratch_shapes=[
            pltpu.VMEM(keep.shape, BF16),
            pltpu.VMEM((2, 2, *half), BF16),
            pltpu.VMEM((2, 2, *half), BF16),
            pltpu.VMEM((2, *half), BF16),
            pltpu.VMEM((2, *half), BF16),
            *extra,
            pltpu.SemaphoreType.DMA((2, n_sems)),
        ],
        compiler_params=pltpu.CompilerParams(
            collective_id=collective_id, has_side_effects=True, vmem_limit_bytes=40 << 20
        ),
        cost_estimate=pl.CostEstimate(
            flops=40_000_000, bytes_accessed=40 << 20, transcendentals=0
        ),
        name=name,
    )(keep, send, *operands)


def on_device(acts, act_mask, w1, cols1, bias1, mask2, w2, cols2, bias2):
    bs = w1.shape[-1]
    rows = acts.shape[0]
    blocks = act_mask.shape[1]
    xh, core, y, xl = (lax.axis_index(a) for a in ("xh", "core", "y", "xl"))
    x = xh * 2 + xl

    w1_all = lax.all_gather(w1, "z", axis=0, tiled=True)
    w2_swapped = lax.ppermute(w2, ("core", "xl"), SWAP)
    w2_all = lax.all_gather(w2_swapped, "z", axis=0, tiled=True)
    cols2 = lax.ppermute(cols2, ("core", "xl"), SWAP)
    bias2 = lax.ppermute(bias2, ("core", "xl"), SWAP)

    live = jnp.repeat(act_mask.astype(BF16), bs, axis=1)
    masked = (acts * live).reshape(rows, 8, 2, 4 * bs)
    mine = lax.dynamic_index_in_dim(masked, xl, 2, keepdims=False).reshape(rows, -1)
    given = lax.dynamic_index_in_dim(masked, 1 - xl, 2, keepdims=False).reshape(rows, -1)
    taken = lax.ppermute(given, "xl", ((0, 1), (1, 0)))
    x0 = jnp.concatenate([jnp.where(xl == 0, mine, taken), jnp.where(xl == 0, taken, mine)], axis=0)

    near1 = lax.dynamic_index_in_dim(cols1.reshape(8, 2, 4, 8), xl, 1, keepdims=False).reshape(32, 8) - y * blocks
    chip1 = near1 // 16
    core1 = lax.rem(near1 // 4, 2)
    block1 = lax.rem(near1 // 8, 2) * 4 + lax.rem(near1, 4)
    pos1 = lax.rem(core1 + core, 2) * 32 + xor4(chip1, x) * 8 + block1
    me = core.astype(jnp.int32).reshape(1)
    keep1, send1 = products(
        x0, w1_all, pos1, me, load_columns, store_columns, (blocks // 2, 2 * rows, bs), 2 * rows, blocks, "layer1"
    )

    live2 = mask2.astype(BF16)
    live2_taken = lax.ppermute(live2, "xl", ((0, 1), (1, 0)))
    live2 = jnp.concatenate(
        [jnp.where(xl == 0, live2, live2_taken), jnp.where(xl == 0, live2_taken, live2)], axis=0
    ).reshape(2 * rows, 4, 2, 2, 4)
    live2 = lax.dynamic_index_in_dim(live2, x, 1, keepdims=False)
    live2 = lax.dynamic_index_in_dim(live2, core, 2, keepdims=False).reshape(2 * rows, 8)
    live2 = jnp.broadcast_to(live2.T[:, :, None], (8, 2 * rows, bs))
    part1 = lax.dynamic_index_in_dim(bias1.reshape(4, 2, 2, 4, bs), x, 0, keepdims=False)
    part1 = lax.dynamic_index_in_dim(part1, core, 1, keepdims=False).reshape(8, bs)
    shape1 = (4, 8, 2 * rows, bs)
    hidden = summed(
        hidden_kernel, keep1.reshape(shape1), send1.reshape(shape1), (part1, live2), shape1, (), 20, 0, "hidden"
    )

    near2 = lax.dynamic_index_in_dim(cols2.reshape(8, 2, 4, 8), core, 1, keepdims=False).reshape(32, 8) - x * blocks
    pos2 = xor4(near2 // 16, y) * 16 + lax.rem(near2, 16)
    keep2, send2 = products(
        hidden.reshape(32, 2 * rows, bs), w2_all, pos2, me, load_blocks, store_rows,
        (blocks, rows, bs), 2 * rows, blocks, "layer2",
    )
    shape2 = (4, 16, rows, bs)
    return summed(
        result_kernel, keep2.reshape(shape2), send2.reshape(shape2), (bias2.reshape(16, bs),),
        (rows, 16 * bs), (pltpu.VMEM((rows, 16 * bs), BF16),), 16, 1, "result",
    )


def solution(mesh):
    finer = Mesh(mesh.devices.reshape(2, 2, mesh.shape["col"], 8, 2), AXES)
    in_specs = (
        P(DEPTH, ROW),
        P(DEPTH, ROW),
        P((*ROW, *DEPTH), "y", None, None),
        P(ROW, "y"),
        P("y"),
        P(DEPTH, "y"),
        P(("y", *DEPTH), ROW, None, None),
        P("y", ROW),
        P((*ROW, "y")),
    )
    out_specs = P(DEPTH, (*ROW, "y"))
    return jax.shard_map(on_device, mesh=finer, in_specs=in_specs, out_specs=out_specs, check_vma=False)
```

```python
import functools

import jax
import jax.numpy as jnp
from jax import lax
from jax.experimental import pallas as pl
from jax.experimental.pallas import tpu as pltpu
from jax.sharding import Mesh
from jax.sharding import PartitionSpec as P

AXES = ("xh", "core", "y", "z", "xl")
DEPTH = ("z", "xl")
ROW = ("xh", "core")
BF16, F32, I32 = jnp.bfloat16, jnp.float32, jnp.int32
MESH = pl.DeviceIdType.MESH
RING = 8
CHUNKS = 4
HOPS = 14
BS = 128
ENTRIES = 8
COLUMNS = 64
ORDER = CHUNKS * RING
NOTHING = ORDER * ENTRIES


def xor(i, j):
    return lax.rem(i // 2 + j // 2, 2) * 2 + lax.rem(i + j, 2)


def greet(devices):
    barrier = pltpu.get_barrier_semaphore()
    for device in devices:
        pl.semaphore_signal(barrier, inc=1, device_id=device, device_id_type=MESH)
    pl.semaphore_wait(barrier, len(devices))


def remote(src, dst, send_sem, recv_sem, device):
    return pltpu.make_async_remote_copy(
        src_ref=src, dst_ref=dst, send_sem=send_sem, recv_sem=recv_sem, device_id=device, device_id_type=MESH
    )


class Ring:
    def __init__(self, shard, whole, z, load_sems, sems):
        self.shard, self.whole, self.z, self.load_sems, self.sems = shard, whole, z, load_sems, sems
        self.to = ({"z": lax.rem(z + 1, RING)}, {"z": lax.rem(z + RING - 1, RING)})

    def chunk(self, way, n, steps):
        behind = n // CHUNKS + steps
        slot = lax.rem(self.z + RING - behind, RING) if way == 0 else lax.rem(self.z + behind, RING)
        c = lax.rem(n, CHUNKS) if way == 0 else lax.rem(n, CHUNKS) + 2 * (n // 12)
        return slot, c

    def hop(self, way, n):
        slot, c = self.chunk(way, n, 0)
        ref = self.whole.at[slot, c]
        return remote(ref, ref, self.sems.at[0, way, n], self.sems.at[1, way, n], self.to[way])

    def start(self):
        for c in range(CHUNKS):
            self.load(c).start()
        for c in range(CHUNKS):
            self.load(c).wait()
            for way in range(2):
                self.hop(way, c).start()

    def load(self, c):
        return pltpu.make_async_copy(self.shard.at[c], self.whole.at[self.z, c], self.load_sems.at[c])

    def pump(self, way, n):
        self.hop(way, n).wait_recv()

        @pl.when(n < (10 if way == 0 else 8))
        def _():
            self.hop(way, n + 4).start()

        if way == 1:

            @pl.when(jnp.logical_and(n >= 10, n < 12))
            def _():
                self.hop(way, n + 2).start()

    def pumps(self, first, last):
        @pl.loop(first, last)
        def _(n):
            for way in range(2):
                self.pump(way, n)

    def end(self):
        @pl.loop(0, HOPS)
        def _(n):
            for way in range(2):
                self.hop(way, n).wait_send()


def write_tables(columns_ref, base, z, parity, table_ref):
    columns = columns_ref[...] - base
    columns = jnp.concatenate([columns, columns], axis=1)
    lane = lax.broadcasted_iota(I32, columns.shape, 1)
    entry = lax.broadcasted_iota(I32, columns.shape, 0)
    last = jnp.full(columns.shape, NOTHING, I32)
    before = jnp.zeros(columns.shape, I32)
    for t in range(ORDER):
        if t < CHUNKS:
            slot, c = z, t
        else:
            n, way = (t - CHUNKS) // 2, (t - CHUNKS) % 2
            steps = n // CHUNKS + 1
            slot = lax.rem(z + (RING - steps if way == 0 else steps), RING)
            c = n % CHUNKS + (2 if way == 1 and n >= 12 else 0)
        row = slot * 8 + parity * CHUNKS + c
        column = jnp.sum(jnp.where(lane == row, columns, 0), axis=1, keepdims=True)
        hit = lane == column
        place = jnp.sum(jnp.where(hit, last, 0), axis=1, keepdims=True)
        before = jnp.where(lane == t, place, before)
        newest = jnp.max(jnp.where(hit, t * ENTRIES + entry, -1), axis=0, keepdims=True)
        last = jnp.where(newest >= 0, newest, last)
    table_ref[pl.ds(0, 8), :] = before
    table_ref[pl.ds(8, 8), :] = last


def use(x_ref, ring, sums, table, slot, c, t):
    lhs = x_ref[slot * CHUNKS + c]
    for k in range(0, ENTRIES, 2):
        rhs = jnp.concatenate([ring.whole[slot, c, k], ring.whole[slot, c, k + 1]], axis=1)
        out = jnp.dot(lhs, rhs, preferred_element_type=F32)
        sums[t * ENTRIES + k] = sums[table[k, t]] + out[:, :BS]
        sums[t * ENTRIES + k + 1] = sums[table[k + 1, t]] + out[:, BS:]


def use_all(x_ref, ring, sums, table, pumped):
    @pl.loop(0, CHUNKS)
    def _(c):
        use(x_ref, ring, sums, table, ring.z, c, c)

    def arrived(n, way):
        slot, c = ring.chunk(way, n, 1)
        use(x_ref, ring, sums, table, slot, c, CHUNKS + 2 * n + way)

    @pl.loop(0, pumped)
    def _(n):
        for way in range(2):
            arrived(n, way)

    @pl.loop(pumped, HOPS)
    def _(n):
        for way in range(2):
            ring.pump(way, n)
        for way in range(2):
            arrived(n, way)


FIRST = ((2, 1), (2, 3))
LANDS = ((3, 0), (1, 0))


def reduce_scatter(other, near, half, source, mine, got, out1, in1, out2, in2, sems, finish, between):
    exchanged = {}
    order = [(2, 0), (2, 1), (1, 0), (3, 1), (3, 0), (1, 1), (0, 0), (0, 1)]
    for n, (g, h) in enumerate(order):
        exchanged[g, h] = remote(
            source(g, h), got.at[g, pl.ds(h * half, half)], sems.at[0, n], sems.at[1, n], other
        )
        exchanged[g, h].start()
    between(0)

    def both(g, h, c):
        return mine(g, h, c) + got[g, h * half + c].astype(F32)

    firsts = {}
    for s in range(2):
        for h in range(2):
            g = FIRST[h][s]
            exchanged[g, h].wait_recv()

            @pl.loop(0, half)
            def _(c):
                out1[h, s, c] = both(g, h, c).astype(BF16)

            n = 8 + 2 * h + s
            firsts[h, s] = remote(out1.at[h, s], in1.at[h, s], sems.at[0, n], sems.at[1, n], near[h])
            firsts[h, s].start()
    between(1)
    seconds = {}
    for h in range(2):
        g = LANDS[h][0]
        exchanged[g, h].wait_recv()
        firsts[h, 0].wait_recv()

        @pl.loop(0, half)
        def _(c):
            out2[h, c] = (both(g, h, c) + in1[h, 0, c].astype(F32)).astype(BF16)

        seconds[h] = remote(out2.at[h], in2.at[h], sems.at[0, 12 + h], sems.at[1, 12 + h], near[1 - h])
        seconds[h].start()
    between(2)
    for h in range(2):
        exchanged[0, h].wait_recv()
        firsts[h, 1].wait_recv()
        seconds[h].wait_recv()
        finish(h, lambda c: both(0, h, c) + in1[h, 1, c].astype(F32) + in2[h, c].astype(F32))
    for copy in [*exchanged.values(), *firsts.values(), *seconds.values()]:
        copy.wait_send()


def first_kernel(
    w1, w2, acts, act_mask, mask2, columns1, columns2, bias2,
    keep, send, w2_out, mask2_out, columns2_out, bias2_out,
    whole, sums, x0, mine, taken, mask_taken, table_v, table,
    load_sems, ring_sems, mine_sems, taken_sems, small_sems, swap_sems, table_sem,
):
    xh, core, y, z, xl = (lax.axis_index(a) for a in AXES)
    x = xh * 2 + xl
    beside = {"xl": 1 - xl}
    home = {"core": 1 - core, "xl": 1 - xl}
    away = xl != core
    ring = Ring(w1, whole, z, load_sems, ring_sems)
    greet((*ring.to, beside, home))
    ring.start()

    def part(s, parity):
        return acts.at[:, pl.ds((s * 8 + parity * CHUNKS) * BS, CHUNKS * BS)]

    def place(ref, s):
        return ref.at[:, pl.ds(s * CHUNKS * BS, CHUNKS * BS)]

    small = [
        remote(act_mask, mask_taken, small_sems.at[0, 0], small_sems.at[1, 0], beside),
        remote(mask2, mask2_out.at[xl], small_sems.at[0, 1], small_sems.at[1, 1], beside),
    ]
    for copy in small:
        copy.start()
    given = [
        remote(part(s, 1 - xl), place(taken, s), taken_sems.at[0, s], taken_sems.at[1, s], beside)
        for s in range(RING)
    ]
    own = [pltpu.make_async_copy(part(s, xl), place(mine, s), mine_sems.at[s]) for s in range(RING)]
    for copy in (*given, *own):
        copy.start()
    moves = ((w2, w2_out), (columns2, columns2_out), (bias2, bias2_out))

    @pl.when(away)
    def _():
        for n, (src, dst) in enumerate(moves):
            remote(src, dst, swap_sems.at[0, n], swap_sems.at[1, n], home).start()

    @pl.when(jnp.logical_not(away))
    def _():
        pltpu.make_async_copy(w2, w2_out, swap_sems.at[0, 0]).start()
        columns2_out[...] = columns2[...]
        bias2_out[...] = bias2[...]

    mask2_out[xl] = mask2[...]
    write_tables(columns1, y * COLUMNS, z, xl, table_v)
    sums[NOTHING] = jnp.zeros(sums.shape[1:], F32)

    def masked(blocks, mask_ref, first_row):
        live = mask_ref[...].astype(F32)
        for i in range(ORDER):
            b = i // CHUNKS * 8 + i % CHUNKS
            column = jnp.where(xl == 0, live[:, b : b + 1], live[:, b + CHUNKS : b + CHUNKS + 1])
            factor = jnp.broadcast_to(column, (live.shape[0], BS)).astype(BF16)
            x0[i, pl.ds(pl.multiple_of(first_row, BS), BS), :] = blocks[:, i * BS : (i + 1) * BS] * factor

    for copy in own:
        copy.wait()
    masked(mine, act_mask, xl * BS)
    to_scalars = pltpu.make_async_copy(table_v, table, table_sem)
    to_scalars.start()
    ring.pumps(0, 3)
    for copy in (*small, *given):
        copy.wait_recv()
    masked(taken, mask_taken, (1 - xl) * BS)
    to_scalars.wait()
    use_all(x0, ring, sums, table, 3)

    for half, ref in enumerate((keep, send)):

        @pl.loop(0, COLUMNS // 2)
        def _(p):
            chip = xor(p // 8, x)
            parity = lax.rem(core + half, 2)
            j = (chip * 2 + lax.rem(p // 4, 2)) * 8 + parity * 4 + lax.rem(p, 4)
            ref[p] = sums[table[8, j]]

    for copy in (*small, *given):
        copy.wait_send()

    @pl.when(away)
    def _():
        for n, (src, dst) in enumerate(moves):
            remote(src, dst, swap_sems.at[0, n], swap_sems.at[1, n], home).wait()

    @pl.when(jnp.logical_not(away))
    def _():
        pltpu.make_async_copy(w2, w2_out, swap_sems.at[0, 0]).wait()

    ring.end()


def second_kernel(
    w2, keep, send, mask2, bias1, columns2, bias2, out,
    whole, sums, hid, live, table_v, table, fin, sent,
    got1, out1a, in1a, out2a, in2a, got2, out1b, in1b, out2b, in2b,
    load_sems, ring_sems, keep_sem, table_sem, sems1, sems2, spread_sems, back_sems,
):
    xh, core, y, z, xl = (lax.axis_index(a) for a in AXES)
    x = xh * 2 + xl
    flip_y = y + 1 - 2 * lax.rem(y, 2)
    other = {"core": 1 - core}
    home = {"core": 1 - core, "xl": 1 - xl}
    away = xl != core
    near_x = ({"xl": 1 - xl}, {"xh": 1 - xh, "xl": 1 - xl})
    chips = (xh * 2 + 1 - xl, 3 - x)
    near_y = ({"y": flip_y}, {"y": 3 - y})
    ring = Ring(w2, whole, z, load_sems, ring_sems)
    greet((*ring.to, other, home, *near_x, *near_y))
    fetch = pltpu.make_async_copy(keep, sums.at[pl.ds(0, COLUMNS // 2)], keep_sem)
    fetch.start()
    ring.start()

    half = 4

    def piece(chip, h):
        return hid.at[pl.ds(chip * 8 + h * half, half)]

    copies = []

    def spread(chip, h, to, n):
        ref = piece(chip, h)
        copy = remote(ref, ref, spread_sems.at[0, n], spread_sems.at[1, n], near_x[to])
        copy.start()
        copies.append(copy)
        return copy

    given = {}

    def finish_hidden(h, total):
        for c in range(half):
            n = h * half + c
            j = (x * 2 + h) * 8 + core * 4 + c
            hid[x * 8 + n] = (jnp.maximum(total(c) + bias1[pl.ds(j, 1), :], 0.0) * live[n].astype(F32)).astype(BF16)
        for to in (1 - h, h):
            given[h, to] = spread(x, h, to, 2 * h + to)

    def between_hidden(stage):
        if stage == 0:
            mask = mask2[...].astype(F32)
            lane = lax.broadcasted_iota(I32, mask.shape[1:], 1)
            for n in range(8):
                j = (x * 2 + n // 4) * 8 + core * 4 + n % 4
                for s in range(2):
                    column = jnp.sum(jnp.where(lane == j, mask[s], 0.0), axis=1, keepdims=True)
                    live[n, s * BS : (s + 1) * BS, :] = jnp.broadcast_to(column, (BS, BS)).astype(BF16)
            fetch.wait()
        elif stage == 1:
            write_tables(columns2, x * COLUMNS, z, core, table_v)
            ring.pumps(0, 1)
        else:
            ring.pumps(1, 3)

    reduce_scatter(
        other, near_x, half,
        lambda g, h: send.at[pl.ds(g * 8 + h * half, half)],
        lambda g, h, c: sums[g * 8 + h * half + c],
        got1, out1a, in1a, out2a, in2a, sems1, finish_hidden, between_hidden,
    )
    to_scalars = pltpu.make_async_copy(table_v, table, table_sem)
    to_scalars.start()
    ring.pumps(3, 5)
    for h in range(2):
        given[h, 1 - h].wait_recv()
        spread(chips[1 - h], h, h, 4 + h)
    ring.pumps(5, 6)
    for h in range(2):
        given[h, h].wait_recv()
    for copy in copies[4:]:
        copy.wait_recv()
    to_scalars.wait()
    sums[NOTHING] = jnp.zeros(sums.shape[1:], F32)
    ring.pumps(6, 8)
    use_all(hid, ring, sums, table, 8)

    half = 8

    def column(g, n):
        return xor(y, g) * 16 + n

    def rows_of(c):
        return pl.ds(pl.multiple_of(c * BS, BS), BS)

    def source(g, h):
        @pl.loop(0, half)
        def _(c):
            n = h * half + c
            sent[g, n] = sums[table[8, column(g, n)], rows_of(1 - core), :].astype(BF16)

        return sent.at[g, pl.ds(h * half, half)]

    def back(h):
        ref = pl.ds(h * half * BS, half * BS)
        return remote(fin.at[:, ref], out.at[:, ref], back_sems.at[0, h], back_sems.at[1, h], home)

    def finish_result(h, total):
        for c in range(half):
            n = h * half + c
            value = jnp.maximum(total(c) + bias2[pl.ds(n, 1), :], 0.0)
            fin[:, n * BS : (n + 1) * BS] = value.astype(BF16)

        @pl.when(away)
        def _():
            back(h).start()

    reduce_scatter(
        other, near_y, half, source,
        lambda g, h, c: sums[table[8, column(g, h * half + c)], rows_of(core), :],
        got2, out1b, in1b, out2b, in2b, sems2, finish_result, lambda stage: None,
    )

    @pl.when(away)
    def _():
        for h in range(2):
            back(h).wait()

    @pl.when(jnp.logical_not(away))
    def _():
        out[...] = fin[...]

    for copy in copies:
        copy.wait_send()
    ring.end()


ANY = pl.BlockSpec(memory_space=pl.ANY)
VMEM = pl.BlockSpec(memory_space=pltpu.VMEM)


def ring_scratch(rows):
    return (
        pltpu.VMEM((RING, CHUNKS, ENTRIES, BS, BS), BF16),
        pltpu.VMEM((NOTHING + 1, rows, BS), F32),
    )


RING_SEMS = (pltpu.SemaphoreType.DMA((CHUNKS,)), pltpu.SemaphoreType.DMA((2, 2, HOPS)))
TABLES = (pltpu.VMEM((16, 128), I32), pltpu.SMEM((16, 128), I32))


def halving_scratch(blocks, rows, exchanged):
    half = (blocks // 2, rows, BS)
    return (
        pltpu.VMEM((4, blocks, rows, BS), exchanged),
        pltpu.VMEM((2, 2, *half), BF16),
        pltpu.VMEM((2, 2, *half), BF16),
        pltpu.VMEM((2, *half), BF16),
        pltpu.VMEM((2, *half), BF16),
    )


def params(collective_id):
    return pltpu.CompilerParams(collective_id=collective_id, has_side_effects=True, vmem_limit_bytes=67_000_000)


def on_device(acts, act_mask, w1, cols1, bias1, mask2, w2, cols2, bias2):
    n = acts.shape[0]
    dma = pltpu.SemaphoreType.DMA
    shape = jax.ShapeDtypeStruct
    keep, send, w2, mask2, columns2, bias2 = pl.pallas_call(
        first_kernel,
        out_shape=(
            shape((COLUMNS // 2, 2 * n, BS), F32),
            shape((COLUMNS // 2, 2 * n, BS), F32),
            shape(w2.shape, BF16),
            shape((2, *mask2.shape), I32),
            shape((ENTRIES, 64), I32),
            shape((16, BS), F32),
        ),
        in_specs=[ANY, ANY, ANY, VMEM, VMEM, VMEM, VMEM, VMEM],
        out_specs=(VMEM,) * 6,
        scratch_shapes=[
            *ring_scratch(2 * n),
            pltpu.VMEM((ORDER, 2 * n, BS), BF16),
            pltpu.VMEM((n, ORDER * BS), BF16),
            pltpu.VMEM((n, ORDER * BS), BF16),
            pltpu.VMEM(act_mask.shape, I32),
            *TABLES,
            *RING_SEMS,
            dma((RING,)),
            dma((2, RING)),
            dma((2, 2)),
            dma((2, 3)),
            dma(()),
        ],
        compiler_params=params(0),
        name="first",
    )(w1, w2, acts, act_mask, mask2, cols1.T, cols2.T, bias2.reshape(16, BS))
    return pl.pallas_call(
        second_kernel,
        out_shape=shape((n, 16 * BS), BF16),
        in_specs=[ANY, ANY, ANY, VMEM, VMEM, VMEM, VMEM],
        out_specs=VMEM,
        scratch_shapes=[
            *ring_scratch(2 * n),
            pltpu.VMEM((ORDER, 2 * n, BS), BF16),
            pltpu.VMEM((8, 2 * n, BS), BF16),
            *TABLES,
            pltpu.VMEM((n, 16 * BS), BF16),
            pltpu.VMEM((4, 16, n, BS), BF16),
            *halving_scratch(8, 2 * n, F32),
            *halving_scratch(16, n, BF16),
            *RING_SEMS,
            dma(()),
            dma(()),
            dma((2, 14)),
            dma((2, 14)),
            dma((2, 6)),
            dma((2, 2)),
        ],
        compiler_params=params(1),
        name="second",
    )(w2, keep, send, mask2, bias1.reshape(COLUMNS, BS), columns2, bias2)


def solution(mesh):
    finer = Mesh(mesh.devices.reshape(2, 2, mesh.shape["col"], RING, 2), AXES)
    in_specs = (
        P(DEPTH, ROW),
        P(DEPTH, ROW),
        P((*ROW, *DEPTH), "y", None, None),
        P(ROW, "y"),
        P("y"),
        P(DEPTH, "y"),
        P(("y", *DEPTH), ROW, None, None),
        P("y", ROW),
        P((*ROW, "y")),
    )
    out_specs = P(DEPTH, (*ROW, "y"))
    return jax.shard_map(on_device, mesh=finer, in_specs=in_specs, out_specs=out_specs, check_vma=False)
```

```python
import jax
import jax.numpy as jnp
from jax import lax
from jax.experimental import pallas as pl
from jax.experimental.pallas import tpu as pltpu
from jax.sharding import Mesh
from jax.sharding import PartitionSpec as P

AXES = ("xh", "core", "y", "z", "xl")
DEPTH = ("z", "xl")
ROW = ("xh", "core")
BF16, F32, I32 = jnp.bfloat16, jnp.float32, jnp.int32
MESH = pl.DeviceIdType.MESH
RING = 8
CHUNKS = 4
HOPS = 14
BS = 128
ENTRIES = 8
COLUMNS = 64
ORDER = CHUNKS * RING
NOTHING = ORDER * ENTRIES


def xor(i, j):
    return lax.rem(i // 2 + j // 2, 2) * 2 + lax.rem(i + j, 2)


def greet(devices):
    barrier = pltpu.get_barrier_semaphore()
    for device in devices:
        pl.semaphore_signal(barrier, inc=1, device_id=device, device_id_type=MESH)
    pl.semaphore_wait(barrier, len(devices))


def remote(src, dst, send_sem, recv_sem, device):
    return pltpu.make_async_remote_copy(
        src_ref=src, dst_ref=dst, send_sem=send_sem, recv_sem=recv_sem, device_id=device, device_id_type=MESH
    )


class Ring:
    def __init__(self, shard, whole, z, load_sems, sems):
        self.shard, self.whole, self.z, self.load_sems, self.sems = shard, whole, z, load_sems, sems
        self.to = ({"z": lax.rem(z + 1, RING)}, {"z": lax.rem(z + RING - 1, RING)})

    def chunk(self, way, n, steps):
        behind = n // CHUNKS + steps
        slot = lax.rem(self.z + RING - behind, RING) if way == 0 else lax.rem(self.z + behind, RING)
        c = lax.rem(n, CHUNKS) if way == 0 else lax.rem(n, CHUNKS) + 2 * (n // 12)
        return slot, c

    def hop(self, way, n):
        slot, c = self.chunk(way, n, 0)
        ref = self.whole.at[slot, c]
        return remote(ref, ref, self.sems.at[0, way, n], self.sems.at[1, way, n], self.to[way])

    def start(self):
        for c in range(CHUNKS):
            self.load(c).start()
        for c in range(CHUNKS):
            self.load(c).wait()
            for way in range(2):
                self.hop(way, c).start()

    def send_own(self):
        for c in range(CHUNKS):
            for way in range(2):
                self.hop(way, c).start()

    def load(self, c):
        return pltpu.make_async_copy(self.shard.at[c], self.whole.at[self.z, c], self.load_sems.at[c])

    def pump(self, way, n):
        self.hop(way, n).wait_recv()

        @pl.when(n < (10 if way == 0 else 8))
        def _():
            self.hop(way, n + 4).start()

        if way == 1:

            @pl.when(jnp.logical_and(n >= 10, n < 12))
            def _():
                self.hop(way, n + 2).start()

    def pumps(self, first, last):
        @pl.loop(first, last)
        def _(n):
            for way in range(2):
                self.pump(way, n)

    def end(self):
        @pl.loop(0, HOPS)
        def _(n):
            for way in range(2):
                self.hop(way, n).wait_send()


def write_tables(columns_ref, base, z, parity, table_ref):
    columns = columns_ref[...] - base
    columns = jnp.concatenate([columns, columns], axis=1)
    lane = lax.broadcasted_iota(I32, columns.shape, 1)
    entry = lax.broadcasted_iota(I32, columns.shape, 0)
    last = jnp.full(columns.shape, NOTHING, I32)
    before = jnp.zeros(columns.shape, I32)
    for t in range(ORDER):
        if t < CHUNKS:
            slot, c = z, t
        else:
            n, way = (t - CHUNKS) // 2, (t - CHUNKS) % 2
            steps = n // CHUNKS + 1
            slot = lax.rem(z + (RING - steps if way == 0 else steps), RING)
            c = n % CHUNKS + (2 if way == 1 and n >= 12 else 0)
        row = slot * 8 + parity * CHUNKS + c
        column = jnp.sum(jnp.where(lane == row, columns, 0), axis=1, keepdims=True)
        hit = lane == column
        place = jnp.sum(jnp.where(hit, last, 0), axis=1, keepdims=True)
        before = jnp.where(lane == t, place, before)
        newest = jnp.max(jnp.where(hit, t * ENTRIES + entry, -1), axis=0, keepdims=True)
        last = jnp.where(newest >= 0, newest, last)
    table_ref[pl.ds(0, 8), :] = before
    table_ref[pl.ds(8, 8), :] = last


def use(x_ref, ring, sums, table, slot, c, t):
    lhs = x_ref[slot * CHUNKS + c]
    for k in range(0, ENTRIES, 2):
        rhs = jnp.concatenate([ring.whole[slot, c, k], ring.whole[slot, c, k + 1]], axis=1)
        out = jnp.dot(lhs, rhs, preferred_element_type=F32)
        sums[t * ENTRIES + k] = sums[table[k, t]] + out[:, :BS]
        sums[t * ENTRIES + k + 1] = sums[table[k + 1, t]] + out[:, BS:]


def use_own(x_ref, ring, sums, table):
    @pl.loop(0, CHUNKS)
    def _(c):
        use(x_ref, ring, sums, table, ring.z, c, c)


def use_arrived(x_ref, ring, sums, table, first, last, pumped):
    @pl.loop(first, last)
    def _(n):
        if not pumped:
            for way in range(2):
                ring.pump(way, n)
        for way in range(2):
            slot, c = ring.chunk(way, n, 1)
            use(x_ref, ring, sums, table, slot, c, CHUNKS + 2 * n + way)


FIRST = ((2, 1), (2, 3))
LANDS = ((3, 0), (1, 0))
UNITS = 16
PART = 4


def reduce_scatter(other, near, mine, theirs, sent, got, out1, in1, out2, in2, sems, finish, between):
    def start(n, src, dst, device):
        copy = remote(src, dst, sems.at[0, n], sems.at[1, n], device)
        copy.start()
        return copy

    def unit(h, s, c):
        return (2 * h + s) * PART + c

    exchanged, firsts, seconds = {}, {}, {}
    order = [(2, 0), (2, 1), (1, 0), (3, 1), (3, 0), (1, 1), (0, 0), (0, 1)]
    for s in range(2):
        for g, h in order:

            @pl.loop(0, PART)
            def _(c):
                n = unit(h, s, c)
                sent[g, n] = theirs(g, n).astype(BF16)

            ref = pl.ds(unit(h, s, 0), PART)
            exchanged[g, h, s] = start(len(exchanged), sent.at[g, ref], got.at[g, ref], other)
    between(0)

    def both(g, h, s, c):
        n = unit(h, s, c)
        return mine(g, n) + got[g, n].astype(F32)

    def first(s, step):
        for h in range(2):
            g = FIRST[h][step]
            exchanged[g, h, s].wait_recv()

            @pl.loop(0, PART)
            def _(c):
                out1[h, step, s, c] = both(g, h, s, c).astype(BF16)

            n = 16 + 4 * s + 2 * step + h
            firsts[h, s, step] = start(n, out1.at[h, step, s], in1.at[h, step, s], near[h])

    def second(s):
        for h in range(2):
            g = LANDS[h][0]
            exchanged[g, h, s].wait_recv()
            firsts[h, s, 0].wait_recv()

            @pl.loop(0, PART)
            def _(c):
                out2[h, s, c] = (both(g, h, s, c) + in1[h, 0, s, c].astype(F32)).astype(BF16)

            seconds[h, s] = start(24 + 2 * s + h, out2.at[h, s], in2.at[h, s], near[1 - h])

    first(0, 0)
    first(0, 1)
    first(1, 0)
    between(1)
    second(0)
    first(1, 1)
    second(1)
    between(2)
    for s in range(2):
        for h in range(2):
            exchanged[0, h, s].wait_recv()
            firsts[h, s, 1].wait_recv()
            seconds[h, s].wait_recv()
            finish(
                h, s, lambda c: both(0, h, s, c) + in1[h, 1, s, c].astype(F32) + in2[h, s, c].astype(F32)
            )
    for copy in [*exchanged.values(), *firsts.values(), *seconds.values()]:
        copy.wait_send()


def kernel(
    w1, w2, acts, act_mask, mask2, columns1, columns2, bias1, bias2, out,
    whole1, whole2, sums, x0, live, mask_taken, masks2, columns_in, bias_in, table_v1, table_v2, table1, table2,
    sent, out1, out2, got_a, in1_a, in2_a, got_b, in1_b, in2_b, fin,
    load_sems, ring1_sems, ring2_sems, mine_sems, taken_sems, small_sems, swap_sems, table_sems,
    sems_a, sems_b, spread_sems, back_sems,
):
    xh, core, y, z, xl = (lax.axis_index(a) for a in AXES)
    x = xh * 2 + xl
    other = {"core": 1 - core}
    home = {"core": 1 - core, "xl": 1 - xl}
    away = xl != core
    near_x = ({"xl": 1 - xl}, {"xh": 1 - xh, "xl": 1 - xl})
    chips = (xh * 2 + 1 - xl, 3 - x)
    near_y = ({"y": y + 1 - 2 * lax.rem(y, 2)}, {"y": 3 - y})
    beside = near_x[0]
    ring1 = Ring(w1, whole1, z, load_sems, ring1_sems)
    ring2 = Ring(w2, whole2, z, load_sems, ring2_sems)
    greet((*ring1.to, other, home, *near_x, *near_y))

    def rows_of(c):
        return pl.ds(pl.multiple_of(c * BS, BS), BS)

    ring1.start()
    small = [
        remote(act_mask, mask_taken, small_sems.at[0, 0], small_sems.at[1, 0], beside),
        remote(mask2, masks2.at[xl], small_sems.at[0, 1], small_sems.at[1, 1], beside),
    ]
    for copy in small:
        copy.start()

    def block(i, parity):
        b = i // CHUNKS * 8 + parity * CHUNKS + lax.rem(i, CHUNKS)
        return acts.at[:, pl.ds(pl.multiple_of(b * BS, BS), BS)]

    def given(i):
        return remote(block(i, 1 - xl), x0.at[i, rows_of(xl)], taken_sems.at[0, i], taken_sems.at[1, i], beside)

    def own(i):
        return pltpu.make_async_copy(block(i, xl), x0.at[i, rows_of(xl)], mine_sems.at[i])

    @pl.loop(0, ORDER)
    def _(i):
        given(i).start()
        own(i).start()

    moves = ((columns2, columns_in), (bias2, bias_in), (w2, whole2.at[z]))

    def swaps():
        return [remote(src, dst, swap_sems.at[0, n], swap_sems.at[1, n], home) for n, (src, dst) in enumerate(moves)]

    def stay():
        return pltpu.make_async_copy(w2, whole2.at[z], swap_sems.at[0, 2])

    @pl.when(away)
    def _():
        for copy in swaps():
            copy.start()

    @pl.when(jnp.logical_not(away))
    def _():
        stay().start()
        columns_in[...] = columns2[...]
        bias_in[...] = bias2[...]

    masks2[xl] = mask2[...]
    write_tables(columns1, y * COLUMNS, z, xl, table_v1)
    sums[NOTHING] = jnp.zeros(sums.shape[1:], F32)

    def by_rows(mask):
        mask = mask.astype(F32)
        return jnp.concatenate([mask, mask], axis=0).T

    def masked(mask_ref, rows):
        factors = by_rows(mask_ref[...])
        for i in range(ORDER):
            b = i // CHUNKS * 8 + i % CHUNKS
            column = jnp.where(xl == 0, factors[:, b : b + 1], factors[:, b + CHUNKS : b + CHUNKS + 1])
            factor = jnp.broadcast_to(column, (BS, BS)).astype(BF16)
            x0[i, rows, :] = x0[i, rows, :] * factor

    @pl.loop(0, ORDER)
    def _(i):
        own(i).wait()

    masked(act_mask, rows_of(xl))
    to_scalars1 = pltpu.make_async_copy(table_v1, table1, table_sems.at[0])
    to_scalars1.start()
    ring1.pumps(0, 3)
    for copy in small:
        copy.wait_recv()

    @pl.loop(0, ORDER)
    def _(i):
        given(i).wait_recv()

    masked(mask_taken, rows_of(1 - xl))
    to_scalars1.wait()

    use_own(x0, ring1, sums, table1)
    use_arrived(x0, ring1, sums, table1, 0, 3, True)
    use_arrived(x0, ring1, sums, table1, 3, 5, False)
    for s in range(2):
        rows = by_rows(masks2[s])
        lane = lax.broadcasted_iota(I32, rows.shape, 1)
        for n in range(8):
            j = (x * 2 + n // 4) * 8 + core * 4 + n % 4
            column = jnp.sum(jnp.where(lane == j, rows, 0.0), axis=1, keepdims=True)
            live[2 * n + s] = jnp.broadcast_to(column, (BS, BS)).astype(BF16)

    @pl.when(away)
    def _():
        for copy in swaps():
            copy.wait_recv()

    @pl.when(jnp.logical_not(away))
    def _():
        stay().wait()

    write_tables(columns_in, x * COLUMNS, z, core, table_v2)
    use_arrived(x0, ring1, sums, table1, 5, 12, False)
    ring2.send_own()
    to_scalars2 = pltpu.make_async_copy(table_v2, table2, table_sems.at[1])
    to_scalars2.start()
    use_arrived(x0, ring1, sums, table1, 12, HOPS, False)

    def hidden_sum(parity):
        def unit(g, n):
            j = (xor(g, x) * 2 + n // 8) * 8 + parity * 4 + lax.rem(n // 2, 4)
            return sums[table1[8, j], rows_of(lax.rem(n, 2)), :]

        return unit

    def piece(chip, h, s):
        return x0.at[pl.ds(chip * 8 + h * 4 + s * 2, 2)]

    copies, spreads = [], {}

    def spread(chip, h, s, to):
        ref, n = piece(chip, h, s), len(copies)
        copy = remote(ref, ref, spread_sems.at[0, n], spread_sems.at[1, n], near_x[to])
        copy.start()
        copies.append(copy)
        return copy

    def finish_hidden(h, s, total):
        for c in range(PART):
            n = (2 * h + s) * PART + c
            j = (x * 2 + n // 8) * 8 + core * 4 + n // 2 % 4
            value = jnp.maximum(total(c) + bias1[pl.ds(j, 1), :], 0.0) * live[n].astype(F32)
            x0[x * 8 + n // 2, pl.ds(n % 2 * BS, BS), :] = value.astype(BF16)
        for to in (1 - h, h):
            spreads[h, s, to] = spread(x, h, s, to)

    def between_hidden(stage):
        if stage > 0:
            ring2.pumps(stage - 1, stage)

    reduce_scatter(
        other, near_x, hidden_sum(core), hidden_sum(1 - core), sent, got_a, out1, in1_a, out2, in2_a, sems_a,
        finish_hidden, between_hidden,
    )
    ring2.pumps(2, 4)
    last = []
    for s in range(2):
        for h in range(2):
            spreads[h, s, 1 - h].wait_recv()
            last.append(spread(chips[1 - h], h, s, h))
    ring2.pumps(4, 6)
    for s in range(2):
        for h in range(2):
            spreads[h, s, h].wait_recv()
    for copy in last:
        copy.wait_recv()
    to_scalars2.wait()

    use_own(x0, ring2, sums, table2)
    use_arrived(x0, ring2, sums, table2, 0, 6, True)
    use_arrived(x0, ring2, sums, table2, 6, HOPS, False)

    def result_sum(half):
        def unit(g, n):
            return sums[table2[8, xor(g, y) * UNITS + n], rows_of(half), :]

        return unit

    def back(h, s):
        ref, n = pl.ds((2 * h + s) * PART * BS, PART * BS), 2 * h + s
        return remote(fin.at[:, ref], out.at[:, ref], back_sems.at[0, n], back_sems.at[1, n], home)

    def finish_result(h, s, total):
        for c in range(PART):
            n = (2 * h + s) * PART + c
            value = jnp.maximum(total(c) + bias_in[pl.ds(n, 1), :], 0.0)
            fin[:, n * BS : (n + 1) * BS] = value.astype(BF16)

        @pl.when(away)
        def _():
            back(h, s).start()

    reduce_scatter(
        other, near_y, result_sum(core), result_sum(1 - core), sent, got_b, out1, in1_b, out2, in2_b, sems_b,
        finish_result, lambda stage: None,
    )

    @pl.when(away)
    def _():
        for s in range(2):
            for h in range(2):
                back(h, s).wait()
        for copy in swaps():
            copy.wait_send()

    @pl.when(jnp.logical_not(away))
    def _():
        out[...] = fin[...]

    @pl.loop(0, ORDER)
    def _(i):
        given(i).wait_send()

    for copy in (*small, *copies):
        copy.wait_send()
    ring1.end()
    ring2.end()


ANY = pl.BlockSpec(memory_space=pl.ANY)
VMEM = pl.BlockSpec(memory_space=pltpu.VMEM)


def on_device(acts, act_mask, w1, cols1, bias1, mask2, w2, cols2, bias2):
    n = acts.shape[0]
    dma = pltpu.SemaphoreType.DMA
    whole = pltpu.VMEM((RING, CHUNKS, ENTRIES, BS, BS), BF16)
    tiles = lambda *count: pltpu.VMEM((*count, BS, BS), BF16)
    table_v, table = pltpu.VMEM((16, 128), I32), pltpu.SMEM((16, 128), I32)
    arrivals = (tiles(4, UNITS), tiles(2, 2, 2, PART), tiles(2, 2, PART))
    return pl.pallas_call(
        kernel,
        out_shape=jax.ShapeDtypeStruct((n, UNITS * BS), BF16),
        in_specs=[ANY, ANY, ANY, *[VMEM] * 6],
        out_specs=VMEM,
        scratch_shapes=[
            whole,
            whole,
            pltpu.VMEM((NOTHING + 1, 2 * n, BS), F32),
            pltpu.VMEM((ORDER, 2 * n, BS), BF16),
            tiles(UNITS),
            pltpu.VMEM((64, n), I32),
            pltpu.VMEM((2, 64, n), I32),
            pltpu.VMEM((ENTRIES, 64), I32),
            pltpu.VMEM((UNITS, BS), F32),
            table_v,
            table_v,
            table,
            table,
            tiles(4, UNITS),
            tiles(2, 2, 2, PART),
            tiles(2, 2, PART),
            *arrivals,
            *arrivals,
            pltpu.VMEM((n, UNITS * BS), BF16),
            dma((CHUNKS,)),
            dma((2, 2, HOPS)),
            dma((2, 2, HOPS)),
            dma((ORDER,)),
            dma((2, ORDER)),
            dma((2, 2)),
            dma((2, 3)),
            dma((2,)),
            dma((2, 28)),
            dma((2, 28)),
            dma((2, 12)),
            dma((2, 4)),
        ],
        compiler_params=pltpu.CompilerParams(collective_id=0, has_side_effects=True, vmem_limit_bytes=67_043_328),
        name="layers",
    )(
        w1, w2, acts, act_mask.T, mask2.T, cols1.T, cols2.T, bias1.reshape(COLUMNS, BS), bias2.reshape(UNITS, BS)
    )


def solution(mesh):
    finer = Mesh(mesh.devices.reshape(2, 2, mesh.shape["col"], RING, 2), AXES)
    in_specs = (
        P(DEPTH, ROW),
        P(DEPTH, ROW),
        P((*ROW, *DEPTH), "y", None, None),
        P(ROW, "y"),
        P("y"),
        P(DEPTH, "y"),
        P(("y", *DEPTH), ROW, None, None),
        P("y", ROW),
        P((*ROW, "y")),
    )
    out_specs = P(DEPTH, (*ROW, "y"))
    return jax.shard_map(on_device, mesh=finer, in_specs=in_specs, out_specs=out_specs, check_vma=False)
```

```python
import jax
import jax.numpy as jnp
from jax import lax
from jax.experimental import pallas as pl
from jax.experimental.pallas import tpu as pltpu
from jax.sharding import Mesh
from jax.sharding import PartitionSpec as P

AXES = ("xh", "core", "y", "z", "xl")
DEPTH = ("z", "xl")
ROW = ("xh", "core")
BF16, F32, I32 = jnp.bfloat16, jnp.float32, jnp.int32
MESH = pl.DeviceIdType.MESH
RING = 8
CHUNKS = 4
HOPS = 14
BS = 128
ENTRIES = 8
COLUMNS = 64
ORDER = CHUNKS * RING
NOTHING = ORDER * ENTRIES


def xor(i, j):
    return lax.rem(i // 2 + j // 2, 2) * 2 + lax.rem(i + j, 2)


def greet(devices):
    barrier = pltpu.get_barrier_semaphore()
    for device in devices:
        pl.semaphore_signal(barrier, inc=1, device_id=device, device_id_type=MESH)
    pl.semaphore_wait(barrier, len(devices))


def remote(src, dst, send_sem, recv_sem, device):
    return pltpu.make_async_remote_copy(
        src_ref=src, dst_ref=dst, send_sem=send_sem, recv_sem=recv_sem, device_id=device, device_id_type=MESH
    )


class Ring:
    def __init__(self, shard, whole, z, load_sems, sems):
        self.shard, self.whole, self.z, self.load_sems, self.sems = shard, whole, z, load_sems, sems
        self.to = ({"z": lax.rem(z + 1, RING)}, {"z": lax.rem(z + RING - 1, RING)})

    def chunk(self, way, n, steps):
        behind = n // CHUNKS + steps
        slot = lax.rem(self.z + RING - behind, RING) if way == 0 else lax.rem(self.z + behind, RING)
        c = lax.rem(n, CHUNKS) if way == 0 else lax.rem(n, CHUNKS) + 2 * (n // 12)
        return slot, c

    def hop(self, way, n):
        slot, c = self.chunk(way, n, 0)
        ref = self.whole.at[slot, c]
        return remote(ref, ref, self.sems.at[0, way, n], self.sems.at[1, way, n], self.to[way])

    def start_loads(self):
        for c in range(CHUNKS):
            self.load(c).start()

    def start(self):
        for c in range(CHUNKS):
            self.load(c).wait()
            for way in range(2):
                self.hop(way, c).start()

    def send_own(self):
        for c in range(CHUNKS):
            for way in range(2):
                self.hop(way, c).start()

    def load(self, c):
        return pltpu.make_async_copy(self.shard.at[c], self.whole.at[self.z, c], self.load_sems.at[c])

    def pump(self, way, n):
        self.hop(way, n).wait_recv()

        @pl.when(n < (10 if way == 0 else 8))
        def _():
            self.hop(way, n + 4).start()

        if way == 1:

            @pl.when(jnp.logical_and(n >= 10, n < 12))
            def _():
                self.hop(way, n + 2).start()

    def pumps(self, first, last):
        @pl.loop(first, last)
        def _(n):
            for way in range(2):
                self.pump(way, n)

    def end(self):
        @pl.loop(0, HOPS)
        def _(n):
            for way in range(2):
                self.hop(way, n).wait_send()


def write_tables(columns_ref, base, z, parity, table_ref):
    columns = columns_ref[...] - base
    columns = jnp.concatenate([columns, columns], axis=1)
    lane = lax.broadcasted_iota(I32, columns.shape, 1)
    entry = lax.broadcasted_iota(I32, columns.shape, 0)
    last = jnp.full(columns.shape, NOTHING, I32)
    before = jnp.zeros(columns.shape, I32)
    for t in range(ORDER):
        if t < CHUNKS:
            slot, c = z, t
        else:
            n, way = (t - CHUNKS) // 2, (t - CHUNKS) % 2
            steps = n // CHUNKS + 1
            slot = lax.rem(z + (RING - steps if way == 0 else steps), RING)
            c = n % CHUNKS + (2 if way == 1 and n >= 12 else 0)
        row = slot * 8 + parity * CHUNKS + c
        column = jnp.sum(jnp.where(lane == row, columns, 0), axis=1, keepdims=True)
        hit = lane == column
        place = jnp.sum(jnp.where(hit, last, 0), axis=1, keepdims=True)
        before = jnp.where(lane == t, place, before)
        newest = jnp.max(jnp.where(hit, t * ENTRIES + entry, -1), axis=0, keepdims=True)
        last = jnp.where(newest >= 0, newest, last)
    table_ref[pl.ds(0, 8), :] = before
    table_ref[pl.ds(8, 8), :] = last


def use(x_ref, ring, sums, table, slot, c, t):
    lhs = x_ref[slot * CHUNKS + c]
    for k in range(0, ENTRIES, 2):
        rhs = jnp.concatenate([ring.whole[slot, c, k], ring.whole[slot, c, k + 1]], axis=1)
        out = jnp.dot(lhs, rhs, preferred_element_type=F32)
        sums[t * ENTRIES + k] = sums[table[k, t]] + out[:, :BS]
        sums[t * ENTRIES + k + 1] = sums[table[k + 1, t]] + out[:, BS:]


def use_own(x_ref, ring, sums, table):
    @pl.loop(0, CHUNKS)
    def _(c):
        use(x_ref, ring, sums, table, ring.z, c, c)


def use_arrived(x_ref, ring, sums, table, first, last, pumped):
    @pl.loop(first, last)
    def _(n):
        if not pumped:
            for way in range(2):
                ring.pump(way, n)
        for way in range(2):
            slot, c = ring.chunk(way, n, 1)
            use(x_ref, ring, sums, table, slot, c, CHUNKS + 2 * n + way)


FIRST = ((2, 1), (2, 3))
LANDS = ((3, 0), (1, 0))
UNITS = 16
PART = 4


def reduce_scatter(other, near, last, mine, theirs, sent, got, out1, in1, out2, in2, sems, keep, finish, between):
    def start(n, src, dst, device):
        copy = remote(src, dst, sems.at[0, n], sems.at[1, n], device)
        copy.start()
        return copy

    def unit(h, s, c):
        return (2 * h + s) * PART + c

    def both(g, h, s, c):
        n = unit(h, s, c)
        return mine(g, n) + got[g, n].astype(F32)

    exchanged, firsts, seconds = {}, {}, {}

    def exchange(s):
        for g, h in [(1, 0), (3, 1), (2, 0), (2, 1), (0, 0), (0, 1), (3, 0), (1, 1)]:
            ref = sent(g, unit(h, s, 0))

            @pl.loop(0, PART)
            def _(c):
                ref[c] = theirs(g, unit(h, s, c)).astype(BF16)

            place = got.at[g, pl.ds(unit(h, s, 0), PART)]
            exchanged[g, h, s] = start(len(exchanged), ref, place, other)

    def first(s, step):
        for h in range(2):
            g = FIRST[h][step]
            exchanged[g, h, s].wait_recv()

            @pl.loop(0, PART)
            def _(c):
                out1[h, step, s, c] = both(g, h, s, c).astype(BF16)

            n = 16 + 4 * s + 2 * step + h
            firsts[h, s, step] = start(n, out1.at[h, step, s], in1.at[h, step, s], near[h])

    def second(s):
        for h in range(2):
            g = LANDS[h][0]
            exchanged[g, h, s].wait_recv()
            firsts[h, s, 0].wait_recv()

            @pl.loop(0, PART)
            def _(c):
                out2[h, s, c] = (both(g, h, s, c) + in1[h, 0, s, c].astype(F32)).astype(BF16)

            seconds[h, s] = start(24 + 2 * s + h, out2.at[h, s], in2.at[h, s], last[1 - h])

    def own(s):
        for h in range(2):
            exchanged[0, h, s].wait_recv()
            firsts[h, s, 1].wait_recv()
            keep(h, s, lambda c: both(0, h, s, c) + in1[h, 1, s, c].astype(F32))

    for s in range(2):
        exchange(s)
        first(s, 1)
        first(s, 0)
    between(0)
    for s in range(2):
        own(s)
        second(s)
    between(1)
    for s in range(2):
        for h in range(2):
            seconds[h, s].wait_recv()
            finish(h, s, lambda c: in2[h, s, c].astype(F32))
    for copy in [*exchanged.values(), *firsts.values(), *seconds.values()]:
        copy.wait_send()


def kernel(
    w1, w2, acts, act_mask, mask2, columns1, columns2, bias1, bias2, out,
    whole1, whole2, sums, x0, live, mask_taken, masks2, columns_in, table_v1, table_v2, table1, table2,
    out1, out2, got_a, in1_a, in2_a, got_b, in1_b, in2_b, kept,
    load_sems, ring1_sems, ring2_sems, mine_sems, taken_sems, small_sems, swap_sems, table_sems,
    sems_a, sems_b, spread_sems, kept_sems,
):
    xh, core, y, z, xl = (lax.axis_index(a) for a in AXES)
    x = xh * 2 + xl
    other = {"core": 1 - core}
    home = {"core": 1 - core, "xl": 1 - xl}
    away = xl != core
    near_x = ({"xl": 1 - xl}, {"xh": 1 - xh, "xl": 1 - xl})
    chips = (xh * 2 + 1 - xl, 3 - x)
    near_y = ({"y": y + 1 - 2 * lax.rem(y, 2)}, {"y": 3 - y})
    last_y = tuple({**near, "core": xl, "xl": core} for near in near_y)
    beside = near_x[0]
    ring1 = Ring(w1, whole1, z, load_sems, ring1_sems)
    ring2 = Ring(w2, whole2, z, load_sems, ring2_sems)

    def rows_of(c):
        return pl.ds(pl.multiple_of(c * BS, BS), BS)

    def block(i, parity):
        b = i // CHUNKS * 8 + parity * CHUNKS + lax.rem(i, CHUNKS)
        return acts.at[:, pl.ds(pl.multiple_of(b * BS, BS), BS)]

    def given(i):
        return remote(block(i, 1 - xl), x0.at[i, rows_of(xl)], taken_sems.at[0, i], taken_sems.at[1, i], beside)

    def own(i):
        return pltpu.make_async_copy(block(i, xl), x0.at[i, rows_of(xl)], mine_sems.at[i])

    ring1.start_loads()

    @pl.loop(0, ORDER)
    def _(i):
        own(i).start()

    greet((*ring1.to, other, home, *near_x, *near_y, *last_y))
    ring1.start()
    small = [
        remote(act_mask, mask_taken, small_sems.at[0, 0], small_sems.at[1, 0], beside),
        remote(mask2, masks2.at[xl], small_sems.at[0, 1], small_sems.at[1, 1], beside),
    ]
    for copy in small:
        copy.start()

    @pl.loop(0, ORDER)
    def _(i):
        given(i).start()

    moves = ((columns2, columns_in), (w2, whole2.at[z]))

    def swaps():
        return [remote(src, dst, swap_sems.at[0, n], swap_sems.at[1, n], home) for n, (src, dst) in enumerate(moves)]

    def stay():
        return pltpu.make_async_copy(w2, whole2.at[z], swap_sems.at[0, 1])

    @pl.when(away)
    def _():
        for copy in swaps():
            copy.start()

    @pl.when(jnp.logical_not(away))
    def _():
        stay().start()
        columns_in[...] = columns2[...]

    masks2[xl] = mask2[...]
    write_tables(columns1, y * COLUMNS, z, xl, table_v1)
    sums[NOTHING] = jnp.zeros(sums.shape[1:], F32)

    def by_rows(mask):
        mask = mask.astype(F32)
        return jnp.concatenate([mask, mask], axis=0).T

    def masked(mask_ref, rows):
        factors = by_rows(mask_ref[...])
        for i in range(ORDER):
            b = i // CHUNKS * 8 + i % CHUNKS
            column = jnp.where(xl == 0, factors[:, b : b + 1], factors[:, b + CHUNKS : b + CHUNKS + 1])
            factor = jnp.broadcast_to(column, (BS, BS)).astype(BF16)
            x0[i, rows, :] = x0[i, rows, :] * factor

    @pl.loop(0, ORDER)
    def _(i):
        own(i).wait()

    masked(act_mask, rows_of(xl))
    to_scalars1 = pltpu.make_async_copy(table_v1, table1, table_sems.at[0])
    to_scalars1.start()
    ring1.pumps(0, 3)
    for copy in small:
        copy.wait_recv()

    @pl.loop(0, ORDER)
    def _(i):
        given(i).wait_recv()

    masked(mask_taken, rows_of(1 - xl))
    to_scalars1.wait()

    use_own(x0, ring1, sums, table1)
    use_arrived(x0, ring1, sums, table1, 0, 3, True)
    use_arrived(x0, ring1, sums, table1, 3, 5, False)
    for s in range(2):
        rows = by_rows(masks2[s])
        lane = lax.broadcasted_iota(I32, rows.shape, 1)
        for n in range(8):
            j = (x * 2 + n // 4) * 8 + core * 4 + n % 4
            column = jnp.sum(jnp.where(lane == j, rows, 0.0), axis=1, keepdims=True)
            live[2 * n + s] = jnp.broadcast_to(column, (BS, BS)).astype(BF16)

    @pl.when(away)
    def _():
        for copy in swaps():
            copy.wait_recv()

    @pl.when(jnp.logical_not(away))
    def _():
        stay().wait()

    write_tables(columns_in, x * COLUMNS, z, core, table_v2)
    use_arrived(x0, ring1, sums, table1, 5, 12, False)
    ring2.send_own()
    to_scalars2 = pltpu.make_async_copy(table_v2, table2, table_sems.at[1])
    to_scalars2.start()
    use_arrived(x0, ring1, sums, table1, 12, HOPS, False)
    ring1.end()

    def sent(g, n):
        return whole1.at[g // 2, g % 2 * 2 + n // 8, pl.ds(n % 8, PART)]

    def hidden_sum(parity):
        def unit(g, n):
            j = (xor(g, x) * 2 + n // 8) * 8 + parity * 4 + lax.rem(n // 2, 4)
            return sums[table1[8, j], rows_of(lax.rem(n, 2)), :]

        return unit

    def piece(chip, h, s):
        return x0.at[pl.ds(chip * 8 + h * 4 + s * 2, 2)]

    copies, spreads = [], {}

    def spread(chip, h, s, to):
        ref, n = piece(chip, h, s), len(copies)
        copy = remote(ref, ref, spread_sems.at[0, n], spread_sems.at[1, n], near_x[to])
        copy.start()
        copies.append(copy)
        return copy

    def keep_hidden(h, s, total):
        @pl.loop(0, PART)
        def _(c):
            kept[0, h, s, c] = total(c)

    def finish_hidden(h, s, rest):
        for c in range(PART):
            n = (2 * h + s) * PART + c
            j = (x * 2 + n // 8) * 8 + core * 4 + n // 2 % 4
            total = kept[0, h, s, c] + rest(c)
            value = jnp.maximum(total + bias1[pl.ds(j, 1), :], 0.0) * live[n].astype(F32)
            x0[x * 8 + n // 2, pl.ds(n % 2 * BS, BS), :] = value.astype(BF16)
        for to in (1 - h, h):
            spreads[h, s, to] = spread(x, h, s, to)

    reduce_scatter(
        other, near_x, near_x, hidden_sum(core), hidden_sum(1 - core), sent, got_a, out1, in1_a, out2, in2_a, sems_a,
        keep_hidden, finish_hidden, lambda stage: ring2.pumps(stage, stage + 1),
    )
    ring2.pumps(2, 4)
    last = []
    for s in range(2):
        for h in range(2):
            spreads[h, s, 1 - h].wait_recv()
            last.append(spread(chips[1 - h], h, s, h))
    ring2.pumps(4, 6)
    for s in range(2):
        for h in range(2):
            spreads[h, s, h].wait_recv()
    for copy in last:
        copy.wait_recv()
    to_scalars2.wait()

    use_own(x0, ring2, sums, table2)
    use_arrived(x0, ring2, sums, table2, 0, 6, True)
    use_arrived(x0, ring2, sums, table2, 6, HOPS, False)

    def result_sum(half):
        def unit(g, n):
            return sums[table2[8, xor(g, y) * UNITS + n], rows_of(half), :]

        return unit

    def send_kept(h, s):
        n = 2 * h + s
        return remote(kept.at[0, h, s], kept.at[1, h, s], kept_sems.at[0, n], kept_sems.at[1, n], home)

    def keep_result(h, s, total):
        @pl.loop(0, PART)
        def _(c):
            kept[0, h, s, c] = total(c)

        @pl.when(away)
        def _():
            send_kept(h, s).start()

    def finish_result(h, s, rest):
        @pl.when(away)
        def _():
            send_kept(h, s).wait_recv()

        for c in range(PART):
            n = (2 * h + s) * PART + c
            total = kept[lax.rem(core + xl, 2), h, s, c] + rest(c)
            out[:, n * BS : (n + 1) * BS] = jnp.maximum(total + bias2[pl.ds(n, 1), :], 0.0).astype(BF16)

    reduce_scatter(
        other, near_y, last_y, result_sum(core), result_sum(1 - core), sent, got_b, out1, in1_b, out2, in2_b, sems_b,
        keep_result, finish_result, lambda stage: None,
    )

    @pl.when(away)
    def _():
        for h in range(2):
            for s in range(2):
                send_kept(h, s).wait_send()
        for copy in swaps():
            copy.wait_send()

    @pl.loop(0, ORDER)
    def _(i):
        given(i).wait_send()

    for copy in (*small, *copies):
        copy.wait_send()
    ring2.end()


ANY = pl.BlockSpec(memory_space=pl.ANY)
VMEM = pl.BlockSpec(memory_space=pltpu.VMEM)


def on_device(acts, act_mask, w1, cols1, bias1, mask2, w2, cols2, bias2):
    n = acts.shape[0]
    dma = pltpu.SemaphoreType.DMA
    whole = pltpu.VMEM((RING, CHUNKS, ENTRIES, BS, BS), BF16)
    tiles = lambda *count: pltpu.VMEM((*count, BS, BS), BF16)
    table_v, table = pltpu.VMEM((16, 128), I32), pltpu.SMEM((16, 128), I32)
    arrivals = (tiles(4, UNITS), tiles(2, 2, 2, PART), tiles(2, 2, PART))
    return pl.pallas_call(
        kernel,
        out_shape=jax.ShapeDtypeStruct((n, UNITS * BS), BF16),
        in_specs=[ANY, ANY, ANY, *[VMEM] * 6],
        out_specs=VMEM,
        scratch_shapes=[
            whole,
            whole,
            pltpu.VMEM((NOTHING + 1, 2 * n, BS), F32),
            pltpu.VMEM((ORDER, 2 * n, BS), BF16),
            tiles(UNITS),
            pltpu.VMEM((64, n), I32),
            pltpu.VMEM((2, 64, n), I32),
            pltpu.VMEM((ENTRIES, 64), I32),
            table_v,
            table_v,
            table,
            table,
            tiles(2, 2, 2, PART),
            tiles(2, 2, PART),
            *arrivals,
            *arrivals,
            pltpu.VMEM((2, 2, 2, PART, BS, BS), F32),
            dma((CHUNKS,)),
            dma((2, 2, HOPS)),
            dma((2, 2, HOPS)),
            dma((ORDER,)),
            dma((2, ORDER)),
            dma((2, 2)),
            dma((2, 2)),
            dma((2,)),
            dma((2, 28)),
            dma((2, 28)),
            dma((2, 12)),
            dma((2, 4)),
        ],
        compiler_params=pltpu.CompilerParams(collective_id=0, has_side_effects=True, vmem_limit_bytes=67_043_328),
        name="layers",
    )(
        w1, w2, acts, act_mask.T, mask2.T, cols1.T, cols2.T, bias1.reshape(COLUMNS, BS), bias2.reshape(UNITS, BS)
    )


def solution(mesh):
    finer = Mesh(mesh.devices.reshape(2, 2, mesh.shape["col"], RING, 2), AXES)
    in_specs = (
        P(DEPTH, ROW),
        P(DEPTH, ROW),
        P((*ROW, *DEPTH), "y", None, None),
        P(ROW, "y"),
        P("y"),
        P(DEPTH, "y"),
        P(("y", *DEPTH), ROW, None, None),
        P("y", ROW),
        P((*ROW, "y")),
    )
    out_specs = P(DEPTH, (*ROW, "y"))
    return jax.shard_map(on_device, mesh=finer, in_specs=in_specs, out_specs=out_specs, check_vma=False)
```

```python
import jax
import jax.numpy as jnp
from jax import lax
from jax.experimental import pallas as pl
from jax.experimental.pallas import tpu as pltpu
from jax.sharding import Mesh
from jax.sharding import PartitionSpec as P

AXES = ("xh", "core", "y", "z", "xl")
DEPTH = ("z", "xl")
ROW = ("xh", "core")
BF16, F32, I32 = jnp.bfloat16, jnp.float32, jnp.int32
MESH = pl.DeviceIdType.MESH
RING = 8
CHUNKS = 4
HOPS = 14
BS = 128
ENTRIES = 8
COLUMNS = 64
ORDER = CHUNKS * RING
NOTHING = ORDER * ENTRIES


def xor(i, j):
    return lax.rem(i // 2 + j // 2, 2) * 2 + lax.rem(i + j, 2)


def greet(devices):
    barrier = pltpu.get_barrier_semaphore()
    for device in devices:
        pl.semaphore_signal(barrier, inc=1, device_id=device, device_id_type=MESH)
    pl.semaphore_wait(barrier, len(devices))


def remote(src, dst, send_sem, recv_sem, device):
    return pltpu.make_async_remote_copy(
        src_ref=src, dst_ref=dst, send_sem=send_sem, recv_sem=recv_sem, device_id=device, device_id_type=MESH
    )


class Ring:
    def __init__(self, shard, whole, z, load_sems, sems):
        self.shard, self.whole, self.z, self.load_sems, self.sems = shard, whole, z, load_sems, sems
        self.to = ({"z": lax.rem(z + 1, RING)}, {"z": lax.rem(z + RING - 1, RING)})

    def chunk(self, way, n, steps):
        behind = n // CHUNKS + steps
        slot = lax.rem(self.z + RING - behind, RING) if way == 0 else lax.rem(self.z + behind, RING)
        c = lax.rem(n, CHUNKS) if way == 0 else lax.rem(n, CHUNKS) + 2 * (n // 12)
        return slot, c

    def hop(self, way, n):
        slot, c = self.chunk(way, n, 0)
        ref = self.whole.at[slot, c]
        return remote(ref, ref, self.sems.at[0, way, n], self.sems.at[1, way, n], self.to[way])

    def start_loads(self):
        for c in range(CHUNKS):
            self.load(c).start()

    def start(self):
        for c in range(CHUNKS):
            self.load(c).wait()
            for way in range(2):
                self.hop(way, c).start()

    def send_own(self):
        for c in range(CHUNKS):
            for way in range(2):
                self.hop(way, c).start()

    def load(self, c):
        return pltpu.make_async_copy(self.shard.at[c], self.whole.at[self.z, c], self.load_sems.at[c])

    def pump(self, way, n):
        self.hop(way, n).wait_recv()

        @pl.when(n < (10 if way == 0 else 8))
        def _():
            self.hop(way, n + 4).start()

        if way == 1:

            @pl.when(jnp.logical_and(n >= 10, n < 12))
            def _():
                self.hop(way, n + 2).start()

    def pumps(self, first, last):
        @pl.loop(first, last)
        def _(n):
            for way in range(2):
                self.pump(way, n)

    def end(self):
        @pl.loop(0, HOPS)
        def _(n):
            for way in range(2):
                self.hop(way, n).wait_send()


def write_tables(columns_ref, base, z, parity, table_ref):
    columns = columns_ref[...] - base
    columns = jnp.concatenate([columns, columns], axis=1)
    lane = lax.broadcasted_iota(I32, columns.shape, 1)
    entry = lax.broadcasted_iota(I32, columns.shape, 0)
    last = jnp.full(columns.shape, NOTHING, I32)
    before = jnp.zeros(columns.shape, I32)
    for t in range(ORDER):
        if t < CHUNKS:
            slot, c = z, t
        else:
            n, way = (t - CHUNKS) // 2, (t - CHUNKS) % 2
            steps = n // CHUNKS + 1
            slot = lax.rem(z + (RING - steps if way == 0 else steps), RING)
            c = n % CHUNKS + (2 if way == 1 and n >= 12 else 0)
        row = slot * 8 + parity * CHUNKS + c
        column = jnp.sum(jnp.where(lane == row, columns, 0), axis=1, keepdims=True)
        hit = lane == column
        place = jnp.sum(jnp.where(hit, last, 0), axis=1, keepdims=True)
        before = jnp.where(lane == t, place, before)
        newest = jnp.max(jnp.where(hit, t * ENTRIES + entry, -1), axis=0, keepdims=True)
        last = jnp.where(newest >= 0, newest, last)
    table_ref[pl.ds(0, 8), :] = before
    table_ref[pl.ds(8, 8), :] = last


def use(x_ref, ring, sums, table, slot, c, t):
    lhs = x_ref[slot * CHUNKS + c]
    for k in range(0, ENTRIES, 2):
        rhs = jnp.concatenate([ring.whole[slot, c, k], ring.whole[slot, c, k + 1]], axis=1)
        out = jnp.dot(lhs, rhs, preferred_element_type=F32)
        sums[t * ENTRIES + k] = sums[table[k, t]] + out[:, :BS]
        sums[t * ENTRIES + k + 1] = sums[table[k + 1, t]] + out[:, BS:]


def use_own(x_ref, ring, sums, table):
    @pl.loop(0, CHUNKS)
    def _(c):
        use(x_ref, ring, sums, table, ring.z, c, c)


def use_arrived(x_ref, ring, sums, table, first, last, pumped):
    @pl.loop(first, last)
    def _(n):
        for way in range(2):
            if not pumped:
                ring.pump(way, n)
            slot, c = ring.chunk(way, n, 1)
            use(x_ref, ring, sums, table, slot, c, CHUNKS + 2 * n + way)


FIRST = ((2, 1), (2, 3))
LANDS = ((3, 0), (1, 0))
UNITS = 16
PART = 4


def reduce_scatter(other, near, last, mine, theirs, sent, got, out1, in1, out2, in2, sems, keep, finish, between):
    def start(n, src, dst, device):
        copy = remote(src, dst, sems.at[0, n], sems.at[1, n], device)
        copy.start()
        return copy

    def unit(h, s, c):
        return (2 * h + s) * PART + c

    def both(g, h, s, c):
        n = unit(h, s, c)
        return mine(g, n) + got[g, n].astype(F32)

    exchanged, firsts, seconds = {}, {}, {}

    def exchange(s):
        for g, h in [(1, 0), (3, 1), (2, 0), (2, 1), (0, 0), (0, 1), (3, 0), (1, 1)]:
            ref = sent(g, unit(h, s, 0))

            @pl.loop(0, PART)
            def _(c):
                ref[c] = theirs(g, unit(h, s, c)).astype(BF16)

            place = got.at[g, pl.ds(unit(h, s, 0), PART)]
            exchanged[g, h, s] = start(len(exchanged), ref, place, other)

    def first(s, step):
        for h in range(2):
            g = FIRST[h][step]
            exchanged[g, h, s].wait_recv()

            @pl.loop(0, PART)
            def _(c):
                out1[h, step, s, c] = both(g, h, s, c).astype(BF16)

            n = 16 + 4 * s + 2 * step + h
            firsts[h, s, step] = start(n, out1.at[h, step, s], in1.at[h, step, s], near[h])

    def second(s):
        for h in range(2):
            g = LANDS[h][0]
            exchanged[g, h, s].wait_recv()
            firsts[h, s, 0].wait_recv()

            @pl.loop(0, PART)
            def _(c):
                out2[h, s, c] = (both(g, h, s, c) + in1[h, 0, s, c].astype(F32)).astype(BF16)

            seconds[h, s] = start(24 + 2 * s + h, out2.at[h, s], in2.at[h, s], last[1 - h])

    def own(s):
        for h in range(2):
            exchanged[0, h, s].wait_recv()
            firsts[h, s, 1].wait_recv()
            keep(h, s, lambda c: both(0, h, s, c) + in1[h, 1, s, c].astype(F32))

    for s in range(2):
        exchange(s)
        first(s, 1)
        first(s, 0)
    between(0)
    for s in range(2):
        own(s)
        second(s)
    between(1)
    for copy in (*exchanged.values(), *firsts.values()):
        copy.wait_send()
    for s in range(2):
        for h in range(2):
            seconds[h, s].wait_recv()
            finish(h, s, lambda c: in2[h, s, c].astype(F32))
    for copy in seconds.values():
        copy.wait_send()


def kernel(
    w1, w2, acts, act_mask, mask2, columns1, columns2, bias1, bias2, out,
    whole1, whole2, sums, x0, live, mask_taken, masks2, columns_in, table_v1, table_v2, table1, table2,
    out1, out2, got_a, in1_a, in2_a, got_b, in1_b, in2_b, kept, kept_out, kept_in,
    load_sems, ring1_sems, ring2_sems, mine_sems, taken_sems, small_sems, swap_sems, table_sems,
    sems_a, sems_b, spread_sems, kept_sems,
):
    xh, core, y, z, xl = (lax.axis_index(a) for a in AXES)
    x = xh * 2 + xl
    other = {"core": 1 - core}
    home = {"core": 1 - core, "xl": 1 - xl}
    away = xl != core
    near_x = ({"xl": 1 - xl}, {"xh": 1 - xh, "xl": 1 - xl})
    chips = (xh * 2 + 1 - xl, 3 - x)
    near_y = ({"y": y + 1 - 2 * lax.rem(y, 2)}, {"y": 3 - y})
    last_y = tuple({**near, "core": xl, "xl": core} for near in near_y)
    beside = near_x[0]
    ring1 = Ring(w1, whole1, z, load_sems, ring1_sems)
    ring2 = Ring(w2, whole2, z, load_sems, ring2_sems)

    def rows_of(c):
        return pl.ds(pl.multiple_of(c * BS, BS), BS)

    def block(i, parity):
        b = i // CHUNKS * 8 + parity * CHUNKS + lax.rem(i, CHUNKS)
        return acts.at[:, pl.ds(pl.multiple_of(b * BS, BS), BS)]

    def given(i):
        return remote(block(i, 1 - xl), x0.at[i, rows_of(xl)], taken_sems.at[0, i], taken_sems.at[1, i], beside)

    def own(i):
        return pltpu.make_async_copy(block(i, xl), x0.at[i, rows_of(xl)], mine_sems.at[i])

    ring1.start_loads()

    @pl.loop(0, ORDER)
    def _(i):
        own(i).start()

    greet((*ring1.to, other, home, *near_x, *near_y, *last_y))
    ring1.start()
    small = [
        remote(act_mask, mask_taken, small_sems.at[0, 0], small_sems.at[1, 0], beside),
        remote(mask2, masks2.at[xl], small_sems.at[0, 1], small_sems.at[1, 1], beside),
    ]
    for copy in small:
        copy.start()

    @pl.loop(0, ORDER)
    def _(i):
        given(i).start()

    moves = ((columns2, columns_in), (w2, whole2.at[z]))

    def swaps():
        return [remote(src, dst, swap_sems.at[0, n], swap_sems.at[1, n], home) for n, (src, dst) in enumerate(moves)]

    def stay():
        return pltpu.make_async_copy(w2, whole2.at[z], swap_sems.at[0, 1])

    @pl.when(away)
    def _():
        for copy in swaps():
            copy.start()

    @pl.when(jnp.logical_not(away))
    def _():
        stay().start()
        columns_in[...] = columns2[...]

    masks2[xl] = mask2[...]
    write_tables(columns1, y * COLUMNS, z, xl, table_v1)
    sums[NOTHING] = jnp.zeros(sums.shape[1:], F32)

    def by_rows(mask):
        mask = mask.astype(F32)
        return jnp.concatenate([mask, mask], axis=0).T

    def masked(mask_ref, rows):
        factors = by_rows(mask_ref[...])
        for i in range(ORDER):
            b = i // CHUNKS * 8 + i % CHUNKS
            column = jnp.where(xl == 0, factors[:, b : b + 1], factors[:, b + CHUNKS : b + CHUNKS + 1])
            factor = jnp.broadcast_to(column, (BS, BS)).astype(BF16)
            x0[i, rows, :] = x0[i, rows, :] * factor

    @pl.loop(0, ORDER)
    def _(i):
        own(i).wait()

    masked(act_mask, rows_of(xl))
    to_scalars1 = pltpu.make_async_copy(table_v1, table1, table_sems.at[0])
    to_scalars1.start()
    ring1.pumps(0, 3)
    for copy in small:
        copy.wait_recv()

    @pl.loop(0, ORDER)
    def _(i):
        given(i).wait_recv()

    masked(mask_taken, rows_of(1 - xl))
    to_scalars1.wait()

    use_own(x0, ring1, sums, table1)
    use_arrived(x0, ring1, sums, table1, 0, 3, True)
    use_arrived(x0, ring1, sums, table1, 3, 5, False)
    for s in range(2):
        rows = by_rows(masks2[s])
        lane = lax.broadcasted_iota(I32, rows.shape, 1)
        for n in range(8):
            j = (x * 2 + n // 4) * 8 + core * 4 + n % 4
            column = jnp.sum(jnp.where(lane == j, rows, 0.0), axis=1, keepdims=True)
            live[2 * n + s] = jnp.broadcast_to(column, (BS, BS)).astype(BF16)

    @pl.when(away)
    def _():
        for copy in swaps():
            copy.wait_recv()

    @pl.when(jnp.logical_not(away))
    def _():
        stay().wait()

    write_tables(columns_in, x * COLUMNS, z, core, table_v2)
    use_arrived(x0, ring1, sums, table1, 5, 12, False)
    ring2.send_own()
    to_scalars2 = pltpu.make_async_copy(table_v2, table2, table_sems.at[1])
    to_scalars2.start()
    use_arrived(x0, ring1, sums, table1, 12, HOPS, False)
    ring1.end()

    def sent(g, n):
        return whole1.at[g // 2, g % 2 * 2 + n // 8, pl.ds(n % 8, PART)]

    def hidden_sum(parity):
        def unit(g, n):
            j = (xor(g, x) * 2 + n // 8) * 8 + parity * 4 + lax.rem(n // 2, 4)
            return sums[table1[8, j], rows_of(lax.rem(n, 2)), :]

        return unit

    def piece(chip, h, s):
        return x0.at[pl.ds(chip * 8 + h * 4 + s * 2, 2)]

    copies, spreads = [], {}

    def spread(chip, h, s, to):
        ref, n = piece(chip, h, s), len(copies)
        copy = remote(ref, ref, spread_sems.at[0, n], spread_sems.at[1, n], near_x[to])
        copy.start()
        copies.append(copy)
        return copy

    def keep_hidden(h, s, total):
        @pl.loop(0, PART)
        def _(c):
            kept[h, s, c] = total(c)

    def finish_hidden(h, s, rest):
        for c in range(PART):
            n = (2 * h + s) * PART + c
            j = (x * 2 + n // 8) * 8 + core * 4 + n // 2 % 4
            total = kept[h, s, c] + rest(c)
            value = jnp.maximum(total + bias1[pl.ds(j, 1), :], 0.0) * live[n].astype(F32)
            x0[x * 8 + n // 2, pl.ds(n % 2 * BS, BS), :] = value.astype(BF16)
        for to in (1 - h, h):
            spreads[h, s, to] = spread(x, h, s, to)

    reduce_scatter(
        other, near_x, near_x, hidden_sum(core), hidden_sum(1 - core), sent, got_a, out1, in1_a, out2, in2_a, sems_a,
        keep_hidden, finish_hidden, lambda stage: ring2.pumps(stage, stage + 1),
    )
    ring2.pumps(2, 4)
    last = []
    for s in range(2):
        for h in range(2):
            spreads[h, s, 1 - h].wait_recv()
            last.append(spread(chips[1 - h], h, s, h))
    ring2.pumps(4, 6)
    for s in range(2):
        for h in range(2):
            spreads[h, s, h].wait_recv()
    for copy in last:
        copy.wait_recv()
    to_scalars2.wait()

    use_own(x0, ring2, sums, table2)
    use_arrived(x0, ring2, sums, table2, 0, 6, True)
    use_arrived(x0, ring2, sums, table2, 6, HOPS, False)

    def result_sum(half):
        def unit(g, n):
            return sums[table2[8, xor(g, y) * UNITS + n], rows_of(half), :]

        return unit

    def send_kept(h, s):
        n = 2 * h + s
        return remote(kept_out.at[h, s], kept_in.at[h, s], kept_sems.at[0, n], kept_sems.at[1, n], home)

    def keep_result(h, s, total):
        @pl.loop(0, PART)
        def _(c):
            value = total(c)
            kept[h, s, c] = value
            kept_out[h, s, c] = value.astype(BF16)

        @pl.when(away)
        def _():
            send_kept(h, s).start()

    def sent_all(stage):
        if stage > 0:
            return

        @pl.loop(0, ORDER)
        def _(i):
            given(i).wait_send()

        @pl.when(away)
        def _():
            for copy in swaps():
                copy.wait_send()

        for copy in (*small, *copies):
            copy.wait_send()
        ring2.end()

    def finish_result(h, s, rest):
        @pl.when(away)
        def _():
            send_kept(h, s).wait_recv()

        for c in range(PART):
            n = (2 * h + s) * PART + c
            total = jnp.where(away, kept_in[h, s, c].astype(F32), kept[h, s, c]) + rest(c)
            out[:, n * BS : (n + 1) * BS] = jnp.maximum(total + bias2[pl.ds(n, 1), :], 0.0).astype(BF16)

    reduce_scatter(
        other, near_y, last_y, result_sum(core), result_sum(1 - core), sent, got_b, out1, in1_b, out2, in2_b, sems_b,
        keep_result, finish_result, sent_all,
    )

    @pl.when(away)
    def _():
        for h in range(2):
            for s in range(2):
                send_kept(h, s).wait_send()


ANY = pl.BlockSpec(memory_space=pl.ANY)
VMEM = pl.BlockSpec(memory_space=pltpu.VMEM)


def on_device(acts, act_mask, w1, cols1, bias1, mask2, w2, cols2, bias2):
    n = acts.shape[0]
    dma = pltpu.SemaphoreType.DMA
    whole = pltpu.VMEM((RING, CHUNKS, ENTRIES, BS, BS), BF16)
    tiles = lambda *count: pltpu.VMEM((*count, BS, BS), BF16)
    table_v, table = pltpu.VMEM((16, 128), I32), pltpu.SMEM((16, 128), I32)
    arrivals = (tiles(4, UNITS), tiles(2, 2, 2, PART), tiles(2, 2, PART))
    return pl.pallas_call(
        kernel,
        out_shape=jax.ShapeDtypeStruct((n, UNITS * BS), BF16),
        in_specs=[ANY, ANY, ANY, *[VMEM] * 6],
        out_specs=VMEM,
        scratch_shapes=[
            whole,
            whole,
            pltpu.VMEM((NOTHING + 1, 2 * n, BS), F32),
            pltpu.VMEM((ORDER, 2 * n, BS), BF16),
            tiles(UNITS),
            pltpu.VMEM((64, n), I32),
            pltpu.VMEM((2, 64, n), I32),
            pltpu.VMEM((ENTRIES, 64), I32),
            table_v,
            table_v,
            table,
            table,
            tiles(2, 2, 2, PART),
            tiles(2, 2, PART),
            *arrivals,
            *arrivals,
            pltpu.VMEM((2, 2, PART, BS, BS), F32),
            tiles(2, 2, PART),
            tiles(2, 2, PART),
            dma((CHUNKS,)),
            dma((2, 2, HOPS)),
            dma((2, 2, HOPS)),
            dma((ORDER,)),
            dma((2, ORDER)),
            dma((2, 2)),
            dma((2, 2)),
            dma((2,)),
            dma((2, 28)),
            dma((2, 28)),
            dma((2, 12)),
            dma((2, 4)),
        ],
        compiler_params=pltpu.CompilerParams(collective_id=0, has_side_effects=True, vmem_limit_bytes=67_043_328),
        name="layers",
    )(
        w1, w2, acts, act_mask.T, mask2.T, cols1.T, cols2.T, bias1.reshape(COLUMNS, BS), bias2.reshape(UNITS, BS)
    )


def solution(mesh):
    finer = Mesh(mesh.devices.reshape(2, 2, mesh.shape["col"], RING, 2), AXES)
    in_specs = (
        P(DEPTH, ROW),
        P(DEPTH, ROW),
        P((*ROW, *DEPTH), "y", None, None),
        P(ROW, "y"),
        P("y"),
        P(DEPTH, "y"),
        P(("y", *DEPTH), ROW, None, None),
        P("y", ROW),
        P((*ROW, "y")),
    )
    out_specs = P(DEPTH, (*ROW, "y"))
    return jax.shard_map(on_device, mesh=finer, in_specs=in_specs, out_specs=out_specs, check_vma=False)
```

```python
import jax
import jax.numpy as jnp
from jax import lax
from jax.experimental import pallas as pl
from jax.experimental.pallas import tpu as pltpu
from jax.sharding import Mesh
from jax.sharding import PartitionSpec as P

AXES = ("xh", "core", "y", "z", "xl")
DEPTH = ("z", "xl")
ROW = ("xh", "core")
BF16, F32, I32 = jnp.bfloat16, jnp.float32, jnp.int32
MESH = pl.DeviceIdType.MESH
RING = 8
CHUNKS = 4
HOPS = 14
BS = 128
ENTRIES = 8
COLUMNS = 64
ORDER = CHUNKS * RING
NOTHING = ORDER * ENTRIES


def xor(i, j):
    return lax.rem(i // 2 + j // 2, 2) * 2 + lax.rem(i + j, 2)


def greet(devices):
    barrier = pltpu.get_barrier_semaphore()
    for device in devices:
        pl.semaphore_signal(barrier, inc=1, device_id=device, device_id_type=MESH)
    pl.semaphore_wait(barrier, len(devices))


def remote(src, dst, send_sem, recv_sem, device):
    return pltpu.make_async_remote_copy(
        src_ref=src, dst_ref=dst, send_sem=send_sem, recv_sem=recv_sem, device_id=device, device_id_type=MESH
    )


class Ring:
    def __init__(self, shard, whole, z, load_sems, sems):
        self.shard, self.whole, self.z, self.load_sems, self.sems = shard, whole, z, load_sems, sems
        self.to = ({"z": lax.rem(z + 1, RING)}, {"z": lax.rem(z + RING - 1, RING)})

    def chunk(self, way, n, steps):
        behind = n // CHUNKS + steps
        slot = lax.rem(self.z + RING - behind, RING) if way == 0 else lax.rem(self.z + behind, RING)
        c = lax.rem(n, CHUNKS) if way == 0 else lax.rem(n, CHUNKS) + 2 * (n // 12)
        return slot, c

    def hop(self, way, n):
        slot, c = self.chunk(way, n, 0)
        ref = self.whole.at[slot, c]
        return remote(ref, ref, self.sems.at[0, way, n], self.sems.at[1, way, n], self.to[way])

    def start_loads(self):
        for c in range(CHUNKS):
            self.load(c).start()

    def start(self):
        for c in range(CHUNKS):
            self.load(c).wait()
            for way in range(2):
                self.hop(way, c).start()

    def send_own(self):
        for c in range(CHUNKS):
            for way in range(2):
                self.hop(way, c).start()

    def load(self, c):
        return pltpu.make_async_copy(self.shard.at[c], self.whole.at[self.z, c], self.load_sems.at[c])

    def pump(self, way, n):
        self.hop(way, n).wait_recv()

        @pl.when(n < (10 if way == 0 else 8))
        def _():
            self.hop(way, n + 4).start()

        if way == 1:

            @pl.when(jnp.logical_and(n >= 10, n < 12))
            def _():
                self.hop(way, n + 2).start()

    def pumps(self, first, last):
        @pl.loop(first, last)
        def _(n):
            for way in range(2):
                self.pump(way, n)

    def end(self):
        @pl.loop(0, HOPS)
        def _(n):
            for way in range(2):
                self.hop(way, n).wait_send()


def write_tables(columns_ref, base, z, parity, table_ref):
    columns = columns_ref[...] - base
    columns = jnp.concatenate([columns, columns], axis=1)
    lane = lax.broadcasted_iota(I32, columns.shape, 1)
    entry = lax.broadcasted_iota(I32, columns.shape, 0)
    last = jnp.full(columns.shape, NOTHING, I32)
    before = jnp.zeros(columns.shape, I32)
    for t in range(ORDER):
        if t < CHUNKS:
            slot, c = z, t
        else:
            n, way = (t - CHUNKS) // 2, (t - CHUNKS) % 2
            steps = n // CHUNKS + 1
            slot = lax.rem(z + (RING - steps if way == 0 else steps), RING)
            c = n % CHUNKS + (2 if way == 1 and n >= 12 else 0)
        row = slot * 8 + parity * CHUNKS + c
        column = jnp.sum(jnp.where(lane == row, columns, 0), axis=1, keepdims=True)
        hit = lane == column
        place = jnp.sum(jnp.where(hit, last, 0), axis=1, keepdims=True)
        before = jnp.where(lane == t, place, before)
        newest = jnp.max(jnp.where(hit, t * ENTRIES + entry, -1), axis=0, keepdims=True)
        last = jnp.where(newest >= 0, newest, last)
    table_ref[pl.ds(0, 8), :] = before
    table_ref[pl.ds(8, 8), :] = last


def use(x_ref, ring, sums, table, slot, c, t):
    lhs = x_ref[slot * CHUNKS + c]
    for k in range(0, ENTRIES, 2):
        rhs = jnp.concatenate([ring.whole[slot, c, k], ring.whole[slot, c, k + 1]], axis=1)
        out = jnp.dot(lhs, rhs, preferred_element_type=F32)
        sums[t * ENTRIES + k] = sums[table[k, t]] + out[:, :BS]
        sums[t * ENTRIES + k + 1] = sums[table[k + 1, t]] + out[:, BS:]


def use_own(x_ref, ring, sums, table):
    @pl.loop(0, CHUNKS)
    def _(c):
        use(x_ref, ring, sums, table, ring.z, c, c)


def use_arrived(x_ref, ring, sums, table, first, last, pumped):
    @pl.loop(first, last)
    def _(n):
        for way in range(2):
            if not pumped:
                ring.pump(way, n)
            slot, c = ring.chunk(way, n, 1)
            use(x_ref, ring, sums, table, slot, c, CHUNKS + 2 * n + way)


FIRST = ((2, 1), (2, 3))
LANDS = ((3, 0), (1, 0))
UNITS = 16
PART = 4


def reduce_scatter(other, near, last, mine, theirs, sent, got, out1, in1, out2, in2, sems, keep, finish, between):
    def start(n, src, dst, device):
        copy = remote(src, dst, sems.at[0, n], sems.at[1, n], device)
        copy.start()
        return copy

    def unit(h, s, c):
        return (2 * h + s) * PART + c

    def both(g, h, s, c):
        n = unit(h, s, c)
        return mine(g, n) + got[g, n].astype(F32)

    exchanged, firsts, seconds = {}, {}, {}

    def exchange(s):
        for g, h in [(1, 0), (3, 1), (2, 0), (2, 1), (0, 0), (0, 1), (3, 0), (1, 1)]:
            ref = sent(g, unit(h, s, 0))

            @pl.loop(0, PART)
            def _(c):
                ref[c] = theirs(g, unit(h, s, c)).astype(BF16)

            place = got.at[g, pl.ds(unit(h, s, 0), PART)]
            exchanged[g, h, s] = start(len(exchanged), ref, place, other)

    def first(s, step):
        for h in range(2):
            g = FIRST[h][step]
            exchanged[g, h, s].wait_recv()

            @pl.loop(0, PART)
            def _(c):
                out1[h, step, s, c] = both(g, h, s, c).astype(BF16)

            n = 16 + 4 * s + 2 * step + h
            firsts[h, s, step] = start(n, out1.at[h, step, s], in1.at[h, step, s], near[h])

    def second(s):
        for h in range(2):
            g = LANDS[h][0]
            exchanged[g, h, s].wait_recv()
            firsts[h, s, 0].wait_recv()

            @pl.loop(0, PART)
            def _(c):
                out2[h, s, c] = (both(g, h, s, c) + in1[h, 0, s, c].astype(F32)).astype(BF16)

            seconds[h, s] = start(24 + 2 * s + h, out2.at[h, s], in2.at[h, s], last[1 - h])

    def own(s):
        for h in range(2):
            exchanged[0, h, s].wait_recv()
            firsts[h, s, 1].wait_recv()
            keep(h, s, lambda c: both(0, h, s, c) + in1[h, 1, s, c].astype(F32))

    for s in range(2):
        exchange(s)
        first(s, 1)
        first(s, 0)
    between(0)
    for s in range(2):
        own(s)
        second(s)
    between(1)
    for copy in (*exchanged.values(), *firsts.values()):
        copy.wait_send()
    for s in range(2):
        for h in range(2):
            seconds[h, s].wait_recv()
            finish(h, s, lambda c: in2[h, s, c].astype(F32))
    for copy in seconds.values():
        copy.wait_send()


def kernel(
    w1, w2, acts, act_mask, mask2, columns1, columns2, bias1_in, bias2_in, out,
    whole1, whole2, sums, x0, live, mask_own, mask_taken, masks2, columns_own, columns_in, bias1, bias2, table_v1, table_v2, table1, table2,
    out1, out2, got_a, in1_a, in2_a, got_b, in1_b, in2_b, kept, kept_out, kept_in,
    load_sems, ring1_sems, ring2_sems, fetch_sems, mine_sems, taken_sems, small_sems, swap_sems, table_sems,
    sems_a, sems_b, spread_sems, kept_sems,
):
    xh, core, y, z, xl = (lax.axis_index(a) for a in AXES)
    x = xh * 2 + xl
    other = {"core": 1 - core}
    home = {"core": 1 - core, "xl": 1 - xl}
    away = xl != core
    near_x = ({"xl": 1 - xl}, {"xh": 1 - xh, "xl": 1 - xl})
    chips = (xh * 2 + 1 - xl, 3 - x)
    near_y = ({"y": y + 1 - 2 * lax.rem(y, 2)}, {"y": 3 - y})
    last_y = tuple({**near, "core": xl, "xl": core} for near in near_y)
    beside = near_x[0]
    ring1 = Ring(w1, whole1, z, load_sems, ring1_sems)
    ring2 = Ring(w2, whole2, z, load_sems, ring2_sems)

    def rows_of(c):
        return pl.ds(pl.multiple_of(c * BS, BS), BS)

    def block(i, parity):
        b = i // CHUNKS * 8 + parity * CHUNKS + lax.rem(i, CHUNKS)
        return acts.at[:, pl.ds(pl.multiple_of(b * BS, BS), BS)]

    def given(i):
        return remote(block(i, 1 - xl), x0.at[i, rows_of(xl)], taken_sems.at[0, i], taken_sems.at[1, i], beside)

    def own(i):
        return pltpu.make_async_copy(block(i, xl), x0.at[i, rows_of(xl)], mine_sems.at[i])

    ring1.start_loads()
    greet((*ring1.to, other, home, *near_x, *near_y))
    ring1.start()
    fetches = [
        pltpu.make_async_copy(src, dst, fetch_sems.at[n])
        for n, (src, dst) in enumerate(
            (
                (columns1, columns_own),
                (act_mask, mask_own),
                (mask2, masks2.at[xl]),
                (bias1_in, bias1),
                (bias2_in, bias2),
            )
        )
    ]
    for copy in fetches:
        copy.start()
    small = [
        remote(act_mask, mask_taken, small_sems.at[0, 0], small_sems.at[1, 0], beside),
        remote(mask2, masks2.at[xl], small_sems.at[0, 1], small_sems.at[1, 1], beside),
    ]
    for copy in small:
        copy.start()

    @pl.loop(0, ORDER)
    def _(i):
        given(i).start()
        own(i).start()

    moves = ((columns2, columns_in), (w2, whole2.at[z]))

    def swaps():
        return [remote(src, dst, swap_sems.at[0, n], swap_sems.at[1, n], home) for n, (src, dst) in enumerate(moves)]

    def stay():
        return [pltpu.make_async_copy(src, dst, swap_sems.at[0, n]) for n, (src, dst) in enumerate(moves)]

    @pl.when(away)
    def _():
        for copy in swaps():
            copy.start()

    @pl.when(jnp.logical_not(away))
    def _():
        for copy in stay():
            copy.start()

    for copy in fetches:
        copy.wait()
    write_tables(columns_own, y * COLUMNS, z, xl, table_v1)
    sums[NOTHING] = jnp.zeros(sums.shape[1:], F32)

    def by_rows(mask):
        mask = mask.astype(F32)
        return jnp.concatenate([mask, mask], axis=0).T

    def masked(mask_ref, rows):
        factors = by_rows(mask_ref[...])
        for i in range(ORDER):
            b = i // CHUNKS * 8 + i % CHUNKS
            column = jnp.where(xl == 0, factors[:, b : b + 1], factors[:, b + CHUNKS : b + CHUNKS + 1])
            factor = jnp.broadcast_to(column, (BS, BS)).astype(BF16)
            x0[i, rows, :] = x0[i, rows, :] * factor

    @pl.loop(0, ORDER)
    def _(i):
        own(i).wait()

    masked(mask_own, rows_of(xl))
    to_scalars1 = pltpu.make_async_copy(table_v1, table1, table_sems.at[0])
    to_scalars1.start()
    ring1.pumps(0, 3)
    for copy in small:
        copy.wait_recv()

    @pl.loop(0, ORDER)
    def _(i):
        given(i).wait_recv()

    masked(mask_taken, rows_of(1 - xl))
    to_scalars1.wait()

    use_own(x0, ring1, sums, table1)
    use_arrived(x0, ring1, sums, table1, 0, 3, True)
    use_arrived(x0, ring1, sums, table1, 3, 5, False)
    for s in range(2):
        rows = by_rows(masks2[s])
        lane = lax.broadcasted_iota(I32, rows.shape, 1)
        for n in range(8):
            j = (x * 2 + n // 4) * 8 + core * 4 + n % 4
            column = jnp.sum(jnp.where(lane == j, rows, 0.0), axis=1, keepdims=True)
            live[2 * n + s] = jnp.broadcast_to(column, (BS, BS)).astype(BF16)

    @pl.when(away)
    def _():
        for copy in swaps():
            copy.wait_recv()

    @pl.when(jnp.logical_not(away))
    def _():
        for copy in stay():
            copy.wait()

    write_tables(columns_in, x * COLUMNS, z, core, table_v2)
    use_arrived(x0, ring1, sums, table1, 5, 12, False)
    ring2.send_own()
    to_scalars2 = pltpu.make_async_copy(table_v2, table2, table_sems.at[1])
    to_scalars2.start()
    use_arrived(x0, ring1, sums, table1, 12, HOPS, False)
    ring1.end()

    def sent(g, n):
        return whole1.at[g // 2, g % 2 * 2 + n // 8, pl.ds(n % 8, PART)]

    def hidden_sum(parity):
        def unit(g, n):
            j = (xor(g, x) * 2 + n // 8) * 8 + parity * 4 + lax.rem(n // 2, 4)
            return sums[table1[8, j], rows_of(lax.rem(n, 2)), :]

        return unit

    def piece(chip, h, s):
        return x0.at[pl.ds(chip * 8 + h * 4 + s * 2, 2)]

    copies, spreads = [], {}

    def spread(chip, h, s, to):
        ref, n = piece(chip, h, s), len(copies)
        copy = remote(ref, ref, spread_sems.at[0, n], spread_sems.at[1, n], near_x[to])
        copy.start()
        copies.append(copy)
        return copy

    def keep_hidden(h, s, total):
        @pl.loop(0, PART)
        def _(c):
            kept[h, s, c] = total(c)

    def finish_hidden(h, s, rest):
        for c in range(PART):
            n = (2 * h + s) * PART + c
            j = (x * 2 + n // 8) * 8 + core * 4 + n // 2 % 4
            total = kept[h, s, c] + rest(c)
            value = jnp.maximum(total + bias1[pl.ds(j, 1), :], 0.0) * live[n].astype(F32)
            x0[x * 8 + n // 2, pl.ds(n % 2 * BS, BS), :] = value.astype(BF16)
        for to in (1 - h, h):
            spreads[h, s, to] = spread(x, h, s, to)

    reduce_scatter(
        other, near_x, near_x, hidden_sum(core), hidden_sum(1 - core), sent, got_a, out1, in1_a, out2, in2_a, sems_a,
        keep_hidden, finish_hidden, lambda stage: ring2.pumps(stage, stage + 1),
    )
    ring2.pumps(2, 4)
    last = []
    for s in range(2):
        for h in range(2):
            spreads[h, s, 1 - h].wait_recv()
            last.append(spread(chips[1 - h], h, s, h))
    ring2.pumps(4, 6)
    for s in range(2):
        for h in range(2):
            spreads[h, s, h].wait_recv()
    for copy in last:
        copy.wait_recv()
    to_scalars2.wait()

    use_own(x0, ring2, sums, table2)
    use_arrived(x0, ring2, sums, table2, 0, 6, True)
    use_arrived(x0, ring2, sums, table2, 6, 10, False)

    @pl.loop(0, ORDER)
    def _(i):
        given(i).wait_send()

    @pl.when(away)
    def _():
        for copy in swaps():
            copy.wait_send()

    for copy in (*small, *copies):
        copy.wait_send()
    use_arrived(x0, ring2, sums, table2, 10, HOPS, False)

    def result_sum(half):
        def unit(g, n):
            return sums[table2[8, xor(g, y) * UNITS + n], rows_of(half), :]

        return unit

    def send_kept(h, s):
        n = 2 * h + s
        return remote(kept_out.at[h, s], kept_in.at[h, s], kept_sems.at[0, n], kept_sems.at[1, n], home)

    def keep_result(h, s, total):
        @pl.loop(0, PART)
        def _(c):
            value = total(c)
            kept[h, s, c] = value
            kept_out[h, s, c] = value.astype(BF16)

        @pl.when(away)
        def _():
            send_kept(h, s).start()

    def finish_result(h, s, rest):
        @pl.when(away)
        def _():
            send_kept(h, s).wait_recv()

        for c in range(PART):
            n = (2 * h + s) * PART + c
            total = jnp.where(away, kept_in[h, s, c].astype(F32), kept[h, s, c]) + rest(c)
            out[:, n * BS : (n + 1) * BS] = jnp.maximum(total + bias2[pl.ds(n, 1), :], 0.0).astype(BF16)

    reduce_scatter(
        other, near_y, last_y, result_sum(core), result_sum(1 - core), sent, got_b, out1, in1_b, out2, in2_b, sems_b,
        keep_result, finish_result, lambda stage: None,
    )

    @pl.when(away)
    def _():
        for h in range(2):
            for s in range(2):
                send_kept(h, s).wait_send()

    ring2.end()


ANY = pl.BlockSpec(memory_space=pl.ANY)
VMEM = pl.BlockSpec(memory_space=pltpu.VMEM)


def on_device(acts, act_mask, w1, cols1, bias1, mask2, w2, cols2, bias2):
    n = acts.shape[0]
    dma = pltpu.SemaphoreType.DMA
    whole = pltpu.VMEM((RING, CHUNKS, ENTRIES, BS, BS), BF16)
    tiles = lambda *count: pltpu.VMEM((*count, BS, BS), BF16)
    table_v, table = pltpu.VMEM((16, 128), I32), pltpu.SMEM((16, 128), I32)
    arrivals = (tiles(4, UNITS), tiles(2, 2, 2, PART), tiles(2, 2, PART))
    return pl.pallas_call(
        kernel,
        out_shape=jax.ShapeDtypeStruct((n, UNITS * BS), BF16),
        in_specs=[ANY] * 9,
        out_specs=VMEM,
        scratch_shapes=[
            whole,
            whole,
            pltpu.VMEM((NOTHING + 1, 2 * n, BS), F32),
            pltpu.VMEM((ORDER, 2 * n, BS), BF16),
            tiles(UNITS),
            pltpu.VMEM((64, n), I32),
            pltpu.VMEM((64, n), I32),
            pltpu.VMEM((2, 64, n), I32),
            pltpu.VMEM((ENTRIES, 64), I32),
            pltpu.VMEM((ENTRIES, 64), I32),
            pltpu.VMEM((COLUMNS, BS), F32),
            pltpu.VMEM((UNITS, BS), F32),
            table_v,
            table_v,
            table,
            table,
            tiles(2, 2, 2, PART),
            tiles(2, 2, PART),
            *arrivals,
            *arrivals,
            pltpu.VMEM((2, 2, PART, BS, BS), F32),
            tiles(2, 2, PART),
            tiles(2, 2, PART),
            dma((CHUNKS,)),
            dma((2, 2, HOPS)),
            dma((2, 2, HOPS)),
            dma((5,)),
            dma((ORDER,)),
            dma((2, ORDER)),
            dma((2, 2)),
            dma((2, 2)),
            dma((2,)),
            dma((2, 28)),
            dma((2, 28)),
            dma((2, 12)),
            dma((2, 4)),
        ],
        compiler_params=pltpu.CompilerParams(collective_id=0, has_side_effects=True, vmem_limit_bytes=67_043_328),
        name="layers",
    )(
        w1, w2, acts, act_mask.T, mask2.T, cols1.T, cols2.T, bias1.reshape(COLUMNS, BS), bias2.reshape(UNITS, BS)
    )


def solution(mesh):
    finer = Mesh(mesh.devices.reshape(2, 2, mesh.shape["col"], RING, 2), AXES)
    in_specs = (
        P(DEPTH, ROW),
        P(DEPTH, ROW),
        P((*ROW, *DEPTH), "y", None, None),
        P(ROW, "y"),
        P("y"),
        P(DEPTH, "y"),
        P(("y", *DEPTH), ROW, None, None),
        P("y", ROW),
        P((*ROW, "y")),
    )
    out_specs = P(DEPTH, (*ROW, "y"))
    return jax.shard_map(on_device, mesh=finer, in_specs=in_specs, out_specs=out_specs, check_vma=False)
```

```python
import jax
import jax.numpy as jnp
from jax import lax
from jax.experimental import pallas as pl
from jax.experimental.pallas import tpu as pltpu
from jax.sharding import Mesh
from jax.sharding import PartitionSpec as P

AXES = ("xh", "core", "y", "z", "xl")
DEPTH = ("z", "xl")
ROW = ("xh", "core")
BF16, F32, I32 = jnp.bfloat16, jnp.float32, jnp.int32
MESH = pl.DeviceIdType.MESH
RING = 8
CHUNKS = 4
HOPS = 14
BS = 128
ENTRIES = 8
COLUMNS = 64
ORDER = CHUNKS * RING
NOTHING = ORDER * ENTRIES


def xor(i, j):
    return lax.rem(i // 2 + j // 2, 2) * 2 + lax.rem(i + j, 2)


def greet(devices):
    barrier = pltpu.get_barrier_semaphore()
    for device in devices:
        pl.semaphore_signal(barrier, inc=1, device_id=device, device_id_type=MESH)
    pl.semaphore_wait(barrier, len(devices))


def remote(src, dst, send_sem, recv_sem, device):
    return pltpu.make_async_remote_copy(
        src_ref=src, dst_ref=dst, send_sem=send_sem, recv_sem=recv_sem, device_id=device, device_id_type=MESH
    )


class Ring:
    def __init__(self, shard, whole, z, load_sems, sems, sent_sem):
        self.shard, self.whole, self.z = shard, whole, z
        self.load_sems, self.sems, self.sent_sem = load_sems, sems, sent_sem
        self.to = ({"z": lax.rem(z + 1, RING)}, {"z": lax.rem(z + RING - 1, RING)})

    def chunk(self, way, n, steps):
        behind = n // CHUNKS + steps
        slot = lax.rem(self.z + RING - behind, RING) if way == 0 else lax.rem(self.z + behind, RING)
        c = lax.rem(n, CHUNKS) if way == 0 else lax.rem(n, CHUNKS) + 2 * (n // 12)
        return slot, c

    def hop(self, way, n):
        slot, c = self.chunk(way, n, 0)
        ref = self.whole.at[slot, c]
        return remote(ref, ref, self.sent_sem, self.sems.at[way, n], self.to[way])

    def start_loads(self):
        for c in range(CHUNKS):
            self.load(c).start()

    def start(self):
        for c in range(CHUNKS):
            self.load(c).wait()
            for way in range(2):
                self.hop(way, c).start()

    def send_own(self):
        for c in range(CHUNKS):
            for way in range(2):
                self.hop(way, c).start()

    def load(self, c):
        return pltpu.make_async_copy(self.shard.at[c], self.whole.at[self.z, c], self.load_sems.at[c])

    def pump(self, way, n):
        self.hop(way, n).wait_recv()

        @pl.when(n < (10 if way == 0 else 8))
        def _():
            self.hop(way, n + 4).start()

        if way == 1:

            @pl.when(jnp.logical_and(n >= 10, n < 12))
            def _():
                self.hop(way, n + 2).start()

    def pumps(self, first, last):
        @pl.loop(first, last)
        def _(n):
            for way in range(2):
                self.pump(way, n)

    def end(self):
        ref = self.whole.at[pl.ds(0, 2 * HOPS // CHUNKS)]
        remote(ref, ref, self.sent_sem, self.sems.at[0, 0], self.to[0]).wait_send()


def write_tables(columns_ref, base, z, parity, table_ref):
    columns = columns_ref[...] - base
    columns = jnp.concatenate([columns, columns], axis=1)
    lane = lax.broadcasted_iota(I32, columns.shape, 1)
    entry = lax.broadcasted_iota(I32, columns.shape, 0)
    last = jnp.full(columns.shape, NOTHING, I32)
    before = jnp.zeros(columns.shape, I32)
    for t in range(ORDER):
        if t < CHUNKS:
            slot, c = z, t
        else:
            n, way = (t - CHUNKS) // 2, (t - CHUNKS) % 2
            steps = n // CHUNKS + 1
            slot = lax.rem(z + (RING - steps if way == 0 else steps), RING)
            c = n % CHUNKS + (2 if way == 1 and n >= 12 else 0)
        row = slot * 8 + parity * CHUNKS + c
        column = jnp.sum(jnp.where(lane == row, columns, 0), axis=1, keepdims=True)
        hit = lane == column
        place = jnp.sum(jnp.where(hit, last, 0), axis=1, keepdims=True)
        before = jnp.where(lane == t, place, before)
        newest = jnp.max(jnp.where(hit, t * ENTRIES + entry, -1), axis=0, keepdims=True)
        last = jnp.where(newest >= 0, newest, last)
    table_ref[pl.ds(0, 8), :] = before
    table_ref[pl.ds(8, 8), :] = last


def use(x_ref, ring, sums, table, slot, c, t):
    lhs = x_ref[slot * CHUNKS + c]
    for k in range(0, ENTRIES, 2):
        rhs = jnp.concatenate([ring.whole[slot, c, k], ring.whole[slot, c, k + 1]], axis=1)
        out = jnp.dot(lhs, rhs, preferred_element_type=F32)
        sums[t * ENTRIES + k] = sums[table[k, t]] + out[:, :BS]
        sums[t * ENTRIES + k + 1] = sums[table[k + 1, t]] + out[:, BS:]


def use_own(x_ref, ring, sums, table):
    @pl.loop(0, CHUNKS)
    def _(c):
        use(x_ref, ring, sums, table, ring.z, c, c)


def use_arrived(x_ref, ring, sums, table, first, last, pumped):
    @pl.loop(first, last)
    def _(n):
        for way in range(2):
            if not pumped:
                ring.pump(way, n)
            slot, c = ring.chunk(way, n, 1)
            use(x_ref, ring, sums, table, slot, c, CHUNKS + 2 * n + way)


FIRST = ((2, 1), (2, 3))
LANDS = ((3, 0), (1, 0))
UNITS = 16
PART = 4


def reduce_scatter(other, near, last, mine, theirs, sent, got, out1, in1, out2, in2, sems, sent_sems, keep, finish, between):
    def start(n, kind, src, dst, device):
        copy = remote(src, dst, sent_sems.at[kind], sems.at[n], device)
        copy.start()
        return copy

    def unit(h, s, c):
        return (2 * h + s) * PART + c

    def both(g, h, s, c):
        n = unit(h, s, c)
        return mine(g, n) + got[g, n].astype(F32)

    exchanged, firsts, seconds = {}, {}, {}

    def exchange(s):
        for g, h in [(1, 0), (3, 1), (2, 0), (2, 1), (0, 0), (0, 1), (3, 0), (1, 1)]:
            ref = sent(g, unit(h, s, 0))

            @pl.loop(0, PART)
            def _(c):
                ref[c] = theirs(g, unit(h, s, c)).astype(BF16)

            place = got.at[g, pl.ds(unit(h, s, 0), PART)]
            exchanged[g, h, s] = start(len(exchanged), 0, ref, place, other)

    def first(s, step):
        for h in range(2):
            g = FIRST[h][step]
            exchanged[g, h, s].wait_recv()

            @pl.loop(0, PART)
            def _(c):
                out1[h, step, s, c] = both(g, h, s, c).astype(BF16)

            n = 16 + 4 * s + 2 * step + h
            firsts[h, s, step] = start(n, 1, out1.at[h, step, s], in1.at[h, step, s], near[h])

    def second(s):
        for h in range(2):
            g = LANDS[h][0]
            exchanged[g, h, s].wait_recv()
            firsts[h, s, 0].wait_recv()

            @pl.loop(0, PART)
            def _(c):
                out2[h, s, c] = (both(g, h, s, c) + in1[h, 0, s, c].astype(F32)).astype(BF16)

            seconds[h, s] = start(24 + 2 * s + h, 2, out2.at[h, s], in2.at[h, s], last[1 - h])

    def own(s):
        for h in range(2):
            exchanged[0, h, s].wait_recv()
            firsts[h, s, 1].wait_recv()
            keep(h, s, lambda c: both(0, h, s, c) + in1[h, 1, s, c].astype(F32))

    for s in range(2):
        exchange(s)
        first(s, 1)
        first(s, 0)
    between(0)
    for s in range(2):
        own(s)
        second(s)
    between(1)

    def all_sent(kind, ref):
        remote(ref, ref, sent_sems.at[kind], sems.at[0], other).wait_send()

    all_sent(0, got)
    all_sent(1, out1)
    for s in range(2):
        for h in range(2):
            seconds[h, s].wait_recv()
            finish(h, s, lambda c: in2[h, s, c].astype(F32))
    all_sent(2, out2)


def kernel(
    w1, w2, acts, act_mask, mask2, columns1, columns2, bias1_in, bias2_in, out,
    whole1, whole2, sums, x0, live, mask_own, mask_taken, masks2, columns_own, columns_in, bias1, bias2, table_v1, table_v2, table1, table2,
    out1, out2, got_a, in1_a, in2_a, got_b, in1_b, in2_b, kept, kept_out, kept_in,
    load_sems, ring1_sems, ring2_sems, ring_sent, fetch_sems, mine_sem, taken_sems, small_sems, swap_sems, table_sems,
    sems_a, sems_b, sent_a, sent_b, spread_sems, kept_sems,
):
    xh, core, y, z, xl = (lax.axis_index(a) for a in AXES)
    x = xh * 2 + xl
    other = {"core": 1 - core}
    home = {"core": 1 - core, "xl": 1 - xl}
    away = xl != core
    near_x = ({"xl": 1 - xl}, {"xh": 1 - xh, "xl": 1 - xl})
    chips = (xh * 2 + 1 - xl, 3 - x)
    near_y = ({"y": y + 1 - 2 * lax.rem(y, 2)}, {"y": 3 - y})
    last_y = tuple({**near, "core": xl, "xl": core} for near in near_y)
    beside = near_x[0]
    ring1 = Ring(w1, whole1, z, load_sems, ring1_sems, ring_sent.at[0])
    ring2 = Ring(w2, whole2, z, load_sems, ring2_sems, ring_sent.at[1])

    def rows_of(c):
        return pl.ds(pl.multiple_of(c * BS, BS), BS)

    def block(i, parity):
        b = i // CHUNKS * 8 + parity * CHUNKS + lax.rem(i, CHUNKS)
        return acts.at[:, pl.ds(pl.multiple_of(b * BS, BS), BS)]

    def given(i):
        return remote(block(i, 1 - xl), x0.at[i, rows_of(xl)], taken_sems.at[0], taken_sems.at[1], beside)

    def own(i):
        return pltpu.make_async_copy(block(i, xl), x0.at[i, rows_of(xl)], mine_sem)

    ring1.start_loads()
    greet((*ring1.to, other, home, *near_x, *near_y))
    ring1.start()
    fetches = [
        pltpu.make_async_copy(src, dst, fetch_sems.at[n])
        for n, (src, dst) in enumerate(
            (
                (columns1, columns_own),
                (act_mask, mask_own),
                (mask2, masks2.at[xl]),
                (bias1_in, bias1),
                (bias2_in, bias2),
            )
        )
    ]
    for copy in fetches:
        copy.start()
    small = [
        remote(act_mask, mask_taken, small_sems.at[0, 0], small_sems.at[1, 0], beside),
        remote(mask2, masks2.at[xl], small_sems.at[0, 1], small_sems.at[1, 1], beside),
    ]
    for copy in small:
        copy.start()

    @pl.loop(0, ORDER)
    def _(i):
        given(i).start()
        own(i).start()

    moves = ((columns2, columns_in), (w2, whole2.at[z]))

    def swaps():
        return [remote(src, dst, swap_sems.at[0, n], swap_sems.at[1, n], home) for n, (src, dst) in enumerate(moves)]

    def stay():
        return [pltpu.make_async_copy(src, dst, swap_sems.at[0, n]) for n, (src, dst) in enumerate(moves)]

    @pl.when(away)
    def _():
        for copy in swaps():
            copy.start()

    @pl.when(jnp.logical_not(away))
    def _():
        for copy in stay():
            copy.start()

    for copy in fetches:
        copy.wait()
    write_tables(columns_own, y * COLUMNS, z, xl, table_v1)
    sums[NOTHING] = jnp.zeros(sums.shape[1:], F32)

    def by_rows(mask):
        mask = mask.astype(F32)
        return jnp.concatenate([mask, mask], axis=0).T

    def masked(mask_ref, rows):
        factors = by_rows(mask_ref[...])
        for i in range(ORDER):
            b = i // CHUNKS * 8 + i % CHUNKS
            column = jnp.where(xl == 0, factors[:, b : b + 1], factors[:, b + CHUNKS : b + CHUNKS + 1])
            factor = jnp.broadcast_to(column, (BS, BS)).astype(BF16)
            x0[i, rows, :] = x0[i, rows, :] * factor

    ref = x0.at[:, rows_of(xl)]
    pltpu.make_async_copy(ref, ref, mine_sem).wait()
    given_all = remote(ref, ref, taken_sems.at[0], taken_sems.at[1], beside)

    masked(mask_own, rows_of(xl))
    to_scalars1 = pltpu.make_async_copy(table_v1, table1, table_sems.at[0])
    to_scalars1.start()
    ring1.pumps(0, 3)
    for copy in small:
        copy.wait_recv()

    given_all.wait_recv()

    masked(mask_taken, rows_of(1 - xl))
    to_scalars1.wait()

    use_own(x0, ring1, sums, table1)
    use_arrived(x0, ring1, sums, table1, 0, 3, True)
    use_arrived(x0, ring1, sums, table1, 3, 5, False)
    for s in range(2):
        rows = by_rows(masks2[s])
        lane = lax.broadcasted_iota(I32, rows.shape, 1)
        for n in range(8):
            j = (x * 2 + n // 4) * 8 + core * 4 + n % 4
            column = jnp.sum(jnp.where(lane == j, rows, 0.0), axis=1, keepdims=True)
            live[2 * n + s] = jnp.broadcast_to(column, (BS, BS)).astype(BF16)

    @pl.when(away)
    def _():
        for copy in swaps():
            copy.wait_recv()

    @pl.when(jnp.logical_not(away))
    def _():
        for copy in stay():
            copy.wait()

    write_tables(columns_in, x * COLUMNS, z, core, table_v2)
    use_arrived(x0, ring1, sums, table1, 5, 12, False)
    ring2.send_own()
    to_scalars2 = pltpu.make_async_copy(table_v2, table2, table_sems.at[1])
    to_scalars2.start()
    use_arrived(x0, ring1, sums, table1, 12, HOPS, False)
    ring1.end()

    def sent(g, n):
        return whole1.at[g // 2, g % 2 * 2 + n // 8, pl.ds(n % 8, PART)]

    def hidden_sum(parity):
        def unit(g, n):
            j = (xor(g, x) * 2 + n // 8) * 8 + parity * 4 + lax.rem(n // 2, 4)
            return sums[table1[8, j], rows_of(lax.rem(n, 2)), :]

        return unit

    def piece(chip, h, s):
        return x0.at[pl.ds(chip * 8 + h * 4 + s * 2, 2)]

    copies, spreads = [], {}

    def spread(chip, h, s, to):
        ref, n = piece(chip, h, s), len(copies)
        copy = remote(ref, ref, spread_sems.at[0, n], spread_sems.at[1, n], near_x[to])
        copy.start()
        copies.append(copy)
        return copy

    def keep_hidden(h, s, total):
        @pl.loop(0, PART)
        def _(c):
            kept[h, s, c] = total(c)

    def finish_hidden(h, s, rest):
        for c in range(PART):
            n = (2 * h + s) * PART + c
            j = (x * 2 + n // 8) * 8 + core * 4 + n // 2 % 4
            total = kept[h, s, c] + rest(c)
            value = jnp.maximum(total + bias1[pl.ds(j, 1), :], 0.0) * live[n].astype(F32)
            x0[x * 8 + n // 2, pl.ds(n % 2 * BS, BS), :] = value.astype(BF16)
        for to in (1 - h, h):
            spreads[h, s, to] = spread(x, h, s, to)

    reduce_scatter(
        other, near_x, near_x, hidden_sum(core), hidden_sum(1 - core), sent, got_a, out1, in1_a, out2, in2_a, sems_a, sent_a,
        keep_hidden, finish_hidden, lambda stage: ring2.pumps(stage, stage + 1),
    )
    ring2.pumps(2, 4)
    last = []
    for s in range(2):
        for h in range(2):
            spreads[h, s, 1 - h].wait_recv()
            last.append(spread(chips[1 - h], h, s, h))
    ring2.pumps(4, 6)
    for s in range(2):
        for h in range(2):
            spreads[h, s, h].wait_recv()
    for copy in last:
        copy.wait_recv()
    to_scalars2.wait()

    use_own(x0, ring2, sums, table2)
    use_arrived(x0, ring2, sums, table2, 0, 6, True)
    use_arrived(x0, ring2, sums, table2, 6, 10, False)

    given_all.wait_send()

    @pl.when(away)
    def _():
        for copy in swaps():
            copy.wait_send()

    for copy in (*small, *copies):
        copy.wait_send()
    use_arrived(x0, ring2, sums, table2, 10, HOPS, False)

    def result_sum(half):
        def unit(g, n):
            return sums[table2[8, xor(g, y) * UNITS + n], rows_of(half), :]

        return unit

    def send_kept(h, s):
        n = 2 * h + s
        return remote(kept_out.at[h, s], kept_in.at[h, s], kept_sems.at[0, n], kept_sems.at[1, n], home)

    def keep_result(h, s, total):
        @pl.loop(0, PART)
        def _(c):
            value = total(c)
            kept[h, s, c] = value
            kept_out[h, s, c] = value.astype(BF16)

        @pl.when(away)
        def _():
            send_kept(h, s).start()

    def finish_result(h, s, rest):
        @pl.when(away)
        def _():
            send_kept(h, s).wait_recv()

        for c in range(PART):
            n = (2 * h + s) * PART + c
            total = jnp.where(away, kept_in[h, s, c].astype(F32), kept[h, s, c]) + rest(c)
            out[:, n * BS : (n + 1) * BS] = jnp.maximum(total + bias2[pl.ds(n, 1), :], 0.0).astype(BF16)

    reduce_scatter(
        other, near_y, last_y, result_sum(core), result_sum(1 - core), sent, got_b, out1, in1_b, out2, in2_b, sems_b, sent_b,
        keep_result, finish_result, lambda stage: None,
    )

    @pl.when(away)
    def _():
        for h in range(2):
            for s in range(2):
                send_kept(h, s).wait_send()

    ring2.end()


ANY = pl.BlockSpec(memory_space=pl.ANY)
VMEM = pl.BlockSpec(memory_space=pltpu.VMEM)


def on_device(acts, act_mask, w1, cols1, bias1, mask2, w2, cols2, bias2):
    n = acts.shape[0]
    dma = pltpu.SemaphoreType.DMA
    whole = pltpu.VMEM((RING, CHUNKS, ENTRIES, BS, BS), BF16)
    tiles = lambda *count: pltpu.VMEM((*count, BS, BS), BF16)
    table_v, table = pltpu.VMEM((16, 128), I32), pltpu.SMEM((16, 128), I32)
    arrivals = (tiles(4, UNITS), tiles(2, 2, 2, PART), tiles(2, 2, PART))
    return pl.pallas_call(
        kernel,
        out_shape=jax.ShapeDtypeStruct((n, UNITS * BS), BF16),
        in_specs=[ANY] * 9,
        out_specs=VMEM,
        scratch_shapes=[
            whole,
            whole,
            pltpu.VMEM((NOTHING + 1, 2 * n, BS), F32),
            pltpu.VMEM((ORDER, 2 * n, BS), BF16),
            tiles(UNITS),
            pltpu.VMEM((64, n), I32),
            pltpu.VMEM((64, n), I32),
            pltpu.VMEM((2, 64, n), I32),
            pltpu.VMEM((ENTRIES, 64), I32),
            pltpu.VMEM((ENTRIES, 64), I32),
            pltpu.VMEM((COLUMNS, BS), F32),
            pltpu.VMEM((UNITS, BS), F32),
            table_v,
            table_v,
            table,
            table,
            tiles(2, 2, 2, PART),
            tiles(2, 2, PART),
            *arrivals,
            *arrivals,
            pltpu.VMEM((2, 2, PART, BS, BS), F32),
            tiles(2, 2, PART),
            tiles(2, 2, PART),
            dma((CHUNKS,)),
            dma((2, HOPS)),
            dma((2, HOPS)),
            dma((2,)),
            dma((5,)),
            dma(()),
            dma((2,)),
            dma((2, 2)),
            dma((2, 2)),
            dma((2,)),
            dma((28,)),
            dma((28,)),
            dma((3,)),
            dma((3,)),
            dma((2, 12)),
            dma((2, 4)),
        ],
        compiler_params=pltpu.CompilerParams(collective_id=0, has_side_effects=True, vmem_limit_bytes=67_043_328),
        name="layers",
    )(
        w1, w2, acts, act_mask.T, mask2.T, cols1.T, cols2.T, bias1.reshape(COLUMNS, BS), bias2.reshape(UNITS, BS)
    )


def solution(mesh):
    finer = Mesh(mesh.devices.reshape(2, 2, mesh.shape["col"], RING, 2), AXES)
    in_specs = (
        P(DEPTH, ROW),
        P(DEPTH, ROW),
        P((*ROW, *DEPTH), "y", None, None),
        P(ROW, "y"),
        P("y"),
        P(DEPTH, "y"),
        P(("y", *DEPTH), ROW, None, None),
        P("y", ROW),
        P((*ROW, "y")),
    )
    out_specs = P(DEPTH, (*ROW, "y"))
    return jax.shard_map(on_device, mesh=finer, in_specs=in_specs, out_specs=out_specs, check_vma=False)
```
